32 devices in a mesh: lat: 2 (over y), lon: 8 (over z, x), lev: 2 (over core).
Axes of the slice: x: 2, y: 2, z: 4, core: 2. Of those that a mesh axis runs over, the one named last changes fastest.
Arguments:
- tokens: bfloat16 [4, 12, 96, 192], P('lev', 'lat', 'lon'), may hold values from -6 to 6
- norm1_gain: float32 [192], replicated, may hold values from 0.8 to 10
- qkv_weight: bfloat16 [192, 576], replicated, may hold values from -0.4375 to 0.4375
- proj_weight: bfloat16 [192, 192], replicated, may hold values from -0.4375 to 0.4375
- earth_bias: bfloat16 [2, 2, 6, 3312], P(None, 'lat'), may hold values from -4 to 4
- norm2_gain: float32 [192], replicated, may hold values from 0.5 to 1.5
- fc1_weight: bfloat16 [192, 768], replicated, may hold values from -0.4375 to 0.4375
- fc2_weight: bfloat16 [768, 192], replicated, may hold values from -0.21875 to 0.21875
Outputs:
- blended: bfloat16 [4, 12, 96, 192], P('lev', 'lat', 'lon')
The draws below stay inside these ranges and needn't reach their ends.
All inputs are finite; a program needn't handle non-finite values.
Results may differ from the reference program's by a relative error of at most 0.008.
The reference program's roundings to bfloat16 on the way count: a program that leaves them out, or rounds other values in their place, can miss the bound.
Values may be sent and summed in bfloat16 or wider, within the bound.
A program may use at most 64 MiB of HBM per device.

```python
import jax
import jax.numpy as jnp
from jax import lax

D = 192
HEADS = 6
FF = 768
WLV = 2
WLA = 6
WLO = 12
POS = 3312
NLEV = 4
NLAT = 12
NLON = 96
NWLEV = 2
NWLAT = 2


def draw_norm1_gain(key, part):
    second_key = jax.random.fold_in(jax.random.fold_in(key, 11), 1)
    return jax.random.uniform(second_key, (D,), jnp.float32, 0.8, 1.25)


def steps_of(own_key, dims, cuts, smallest, high):
    level = 1.0
    for axis_at, parts in cuts:
        draws = jax.random.uniform(jax.random.fold_in(jax.random.fold_in(own_key, 6), axis_at), (parts,), jnp.float32, smallest / len(cuts), high / len(cuts))
        level = level * jnp.repeat(jnp.exp(draws), dims[axis_at] // parts).reshape((-1,) + (1,) * (len(dims) - 1 - axis_at))
    return level


def centred(key, shape, width, limit, shards=(), held_as=jnp.bfloat16):
    loudness = steps_of(key, shape, shards, -0.22, 0.18) if shards else 1.0
    entries = jax.random.normal(key, shape, jnp.float32) * width * loudness
    return jnp.minimum(jnp.maximum(entries, -limit), limit).astype(held_as)


def setup_inputs(seed: int = 0) -> dict:
    splits = jax.random.split(jax.random.key(seed), 9)
    return {
        "tokens": centred(splits[0], (NLEV, NLAT, NLON, D), 1.0, 6.0, ((0, 2), (1, 2), (2, 8))),
        "norm1_gain": draw_norm1_gain(jax.random.fold_in(splits[8], 71), 0),
        "qkv_weight": centred(splits[2], (D, 3 * D), D ** -0.5, 0.4375),
        "proj_weight": centred(splits[3], (D, D), D ** -0.5, 0.4375),
        "earth_bias": centred(splits[4], (NWLEV, NWLAT, HEADS, POS), 1.0, 4.0, ((1, 2),)),
        "norm2_gain": jnp.clip(1.0 + 0.1 * jax.random.normal(splits[5], (D,), jnp.float32), 0.5, 1.5),
        "fc1_weight": centred(splits[6], (D, FF), D ** -0.5, 0.4375),
        "fc2_weight": centred(splits[7], (FF, D), FF ** -0.5, 0.21875),
    }


norm_eps = 1e-05

def layer_norm(values, scale_gain):
    average = lax.optimization_barrier(jnp.mean(values, axis=-1, keepdims=True))
    centered = values - average
    variance = lax.optimization_barrier(jnp.mean(centered * centered, axis=-1, keepdims=True))
    return centered * lax.rsqrt(variance + norm_eps) * scale_gain

def window_coords():
    places = jnp.arange(WLV * WLA * WLO, dtype=jnp.int32)
    return (places // (WLA * WLO), places // WLO % WLA, places % WLO)

def bias_index():
    lev_place, lat_place, lon_place = window_coords()
    paired = (lev_place[:, None] * WLV + lev_place[None, :]) * WLA + lat_place[:, None]
    paired = paired * WLA + lat_place[None, :]
    return (paired * (2 * WLO - 1) + lon_place[:, None] - lon_place[None, :] + WLO - 1).astype(jnp.int32)

def region_of(places, extent, window):
    return jnp.where(places < extent - window, 0, jnp.where(places < extent - window // 2, 1, 2)).astype(jnp.int32)

def attend_windows(windows, qkv_weight, bias_terms, allowed):
    window_count, window_size, feature_width = windows.shape
    head_dim = feature_width // HEADS
    projected = jnp.dot(windows.reshape(window_count * window_size, feature_width), qkv_weight, preferred_element_type=jnp.float32)
    projected = lax.optimization_barrier(projected.astype(jnp.bfloat16))
    projected = projected.reshape(window_count, window_size, 3, HEADS, head_dim).astype(jnp.float32)
    queries = projected[:, :, 0]
    key_rows = projected[:, :, 1]
    value_rows = projected[:, :, 2]
    scores = jnp.einsum('wqhd,wkhd->whqk', queries, key_rows) * head_dim ** (-0.5) + bias_terms
    scores = jnp.where(allowed[:, None], scores, -1e+30)
    row_max = lax.optimization_barrier(jnp.max(scores, axis=-1, keepdims=True))
    weights = jnp.exp(scores - row_max)
    probs = weights / lax.optimization_barrier(jnp.sum(weights, axis=-1, keepdims=True))
    probs = lax.optimization_barrier(probs.astype(jnp.bfloat16))
    context = jnp.einsum('whqk,wkhd->wqhd', probs.astype(jnp.float32), value_rows)
    return context.astype(jnp.bfloat16).reshape(window_count, window_size, feature_width)

def reference(tokens, norm1_gain, qkv_weight, proj_weight, earth_bias, norm2_gain, fc1_weight, fc2_weight):
    half_lev, half_lat, half_lon = (WLV // 2, WLA // 2, WLO // 2)
    normed = layer_norm(tokens.astype(jnp.float32), norm1_gain).astype(jnp.bfloat16)
    rolled = jnp.roll(normed, (-half_lev, -half_lat, -half_lon), axis=(0, 1, 2))
    table_index = bias_index()
    lev_place, lat_place, lon_place = window_coords()
    lon_windows = NLON // WLO
    window_size = WLV * WLA * WLO

    def one_band(flat_index):
        lev_window = flat_index // NWLAT
        lat_window = flat_index % NWLAT
        zero = jnp.zeros((), jnp.int32)
        banded = lax.dynamic_slice(rolled, (lev_window * WLV, lat_window * WLA, zero, zero), (WLV, WLA, NLON, D))
        windows = banded.reshape(WLV, WLA, lon_windows, WLO, D).transpose(2, 0, 1, 3, 4)
        windows = windows.reshape(lon_windows, window_size, D)
        tables = earth_bias[lev_window, lat_window]
        bias_terms = jnp.take(tables, table_index, axis=1).astype(jnp.float32)
        lev_region = region_of(lev_window * WLV + lev_place, NLEV, WLV)
        lat_region = region_of(lat_window * WLA + lat_place, NLAT, WLA)
        allowed = (lev_region[:, None] == lev_region[None, :]) & (lat_region[:, None] == lat_region[None, :])
        context = attend_windows(windows, qkv_weight, bias_terms[None], allowed[None])
        context = context.reshape(lon_windows, WLV, WLA, WLO, D).transpose(1, 2, 0, 3, 4)
        return context.reshape(WLV, WLA, NLON, D)
    bands = lax.map(one_band, jnp.arange(NWLEV * NWLAT, dtype=jnp.int32))
    context = bands.reshape(NWLEV, NWLAT, WLV, WLA, NLON, D).transpose(0, 2, 1, 3, 4, 5)
    context = context.reshape(NLEV, NLAT, NLON, D)
    context = jnp.roll(context, (half_lev, half_lat, half_lon), axis=(0, 1, 2))

    def one_level(paired_level):
        own_level, mixed_level = paired_level
        first = own_level.reshape(-1, D).astype(jnp.float32) + jnp.dot(mixed_level.reshape(-1, D), proj_weight, preferred_element_type=jnp.float32)
        normed_two = layer_norm(first, norm2_gain).astype(jnp.bfloat16)
        hidden = jax.nn.gelu(jnp.dot(normed_two, fc1_weight, preferred_element_type=jnp.float32), approximate=False).astype(jnp.bfloat16)
        result = first + jnp.dot(hidden, fc2_weight, preferred_element_type=jnp.float32)
        return result.astype(jnp.bfloat16).reshape(own_level.shape)
    return lax.map(one_level, (tokens, context))
```

```python
import functools

import jax
import jax.numpy as jnp
import numpy as np
from jax import lax
from jax.experimental import pallas as pl
from jax.experimental.pallas import tpu as pltpu
from jax.sharding import PartitionSpec as P

HEADS = 6
WLV = 2
WLA = 6
WLO = 12
HALF_LA = WLA // 2
HALF_LO = WLO // 2
OCT = HALF_LA * HALF_LO
PITCH = 24
SIDE = 2 * PITCH
LATS = 2 * SIDE
SPAN = 2 * WLO - 1
CHUNK = WLA * SPAN
ROWS = 8
LANES = 128
AXES = ("lev", "lat", "lon")
OPERANDS = 9
STACK = HEADS * PITCH
SECTION = HALF_LA * CHUNK
KINDS = 5

norm_eps = 1e-05


def octant_row(lat, lon):
    return lat // HALF_LA * PITCH + lat % HALF_LA * HALF_LO + lon % HALF_LO


def toeplitz_matrix():
    pick = np.zeros((CHUNK, WLO * LANES), np.float32)
    for lon in range(WLO):
        for key_lat in range(WLA):
            for key_lon in range(WLO):
                column = lon * LANES + key_lon // HALF_LO * SIDE + octant_row(key_lat, key_lon)
                pick[key_lat * SPAN + lon - key_lon + WLO - 1, column] = 1
    return pick


def layer_norm(values, scale_gain):
    average = jnp.mean(values, axis=-1, keepdims=True)
    centered = values - average
    variance = jnp.mean(centered * centered, axis=-1, keepdims=True)
    return centered * lax.rsqrt(variance + norm_eps) * scale_gain


def matmul(a, b):
    return jnp.dot(a, b, preferred_element_type=jnp.float32)


def lat_moves(size, at):
    stay = (0, PITCH, PITCH, SIDE)
    if size == 2:
        source = pl.multiple_of((2 - at) * PITCH, PITCH)
        target = pl.multiple_of(at * 3 * PITCH, PITCH)
        return (stay, (1, source, target, PITCH))
    return (stay, (1, 2 * PITCH, 0, PITCH), (-1, PITCH, 3 * PITCH, PITCH))


def lon_moves():
    return (
        (1, slice(2, 3), slice(0, 1)),
        (-1, slice(1, 2), slice(3, 4)),
        (0, slice(1, 3), slice(1, 3)),
    )


def message_count(sizes):
    lats = len(lat_moves(sizes[1], 0))
    return 4 * lats + (lats - 1) + 3 + 1


def kernel(sizes, *refs):
    operands, out_ref, held = refs[:OPERANDS], refs[OPERANDS], refs[OPERANDS + 1 : -14]
    (
        own,
        cells,
        tables,
        chunks_out,
        chunks_in,
        bias,
        weights,
        stacked,
        keys,
        values,
        rows_out,
        sems,
        load_sems,
        ready,
    ) = refs[-14:]
    loads = [
        pltpu.make_async_copy(source, place, load_sems.at[i])
        for i, (source, place) in enumerate(zip(operands, held))
    ]
    for load in loads:
        load.start()
    (
        tokens_ref,
        gain1_ref,
        table_ref,
        pick_ref,
        qkv_ref,
        proj_ref,
        gain2_ref,
        fc1_ref,
        fc2_ref,
    ) = held
    lev, lat, lon = where = [lax.axis_index(axis) for axis in AXES]
    features = own.shape[-1]
    slots = (lev, 1 - lev)

    def device(steps):
        return {
            axis: lax.rem(at + step + size, size)
            for axis, at, step, size in zip(AXES, where, steps, sizes)
        }

    moves = lat_moves(sizes[1], lat)
    per_side = 2 * len(moves)

    def remote(source, target, index, there):
        return pltpu.make_async_remote_copy(
            src_ref=source,
            dst_ref=target,
            send_sem=sems.at[0, index],
            recv_sem=sems.at[1, index],
            device_id=there,
            device_id_type=pl.DeviceIdType.MESH,
        )

    tail_kinds, plain_kind = slice(1, 3), slice(0, 1)
    first_parts, last_parts, peers = {}, {}, {}
    for side, (lon_step, lon_from, lon_to) in enumerate(lon_moves()[:2]):
        first_parts[lon_step], last_parts[lon_step], peers[lon_step] = [], [], []
        for at, (lat_step, lat_from, lat_to, rows) in enumerate(moves):
            there = device((0, lat_step, lon_step))
            peers[lon_step].append(there)
            for part, kinds in enumerate((tail_kinds, plain_kind)):
                (first_parts, last_parts)[part][lon_step].append(
                    remote(
                        cells.at[lon_from, kinds, pl.ds(lat_from, rows), :],
                        cells.at[lon_to, kinds, pl.ds(lat_to, rows), :],
                        side * per_side + at * 2 + part,
                        there,
                    )
                )
    row_copies, row_peers = [], []
    for at, (lat_step, lat_from, lat_to, rows) in enumerate(moves[1:]):
        row_peers.append(device((0, lat_step, 0)))
        row_copies.append(
            remote(
                cells.at[1:3, 0:3, pl.ds(lat_from, rows), :],
                cells.at[1:3, 0:3, pl.ds(lat_to, rows), :],
                2 * per_side + at,
                row_peers[-1],
            )
        )
    partner = device((1, 0, 0))
    passed = 2 * per_side + len(row_copies)

    def pass_on(columns, index):
        return remote(
            cells.at[columns, 1:3, :, :], cells.at[columns, 3:5, :, :], passed + index, partner
        )

    own_pass = pass_on(slice(1, 3), 2)
    table_copy = remote(chunks_out, chunks_in, passed + 3, device((0, 1, 0)))

    barrier = pltpu.get_barrier_semaphore()
    first_lon, last_lon = lon == 0, lon == sizes[2] - 1

    def tell(semaphore, group):
        for there in group:
            pl.semaphore_signal(
                semaphore, inc=1, device_id=there, device_id_type=pl.DeviceIdType.MESH
            )

    tell(barrier, row_peers + [partner] + peers[-1])
    pl.when(jnp.logical_not(last_lon))(lambda: tell(barrier, peers[1]))
    wrapped = len(moves)
    greetings = len(row_peers) + 1 + 2 * wrapped

    for start in (OCT, PITCH + OCT):
        own[:, :, start : start + PITCH - OCT, :] = jnp.zeros(
            (2, 2, PITCH - OCT, features), jnp.float32
        )
    if sizes[1] == 2:
        blank = jnp.zeros((4, 3, PITCH, LANES), jnp.bfloat16)

        def clear_low():
            cells[:, 0:3, :PITCH, :] = blank

        def clear_high():
            cells[:, 0:3, 3 * PITCH :, :] = blank

        pl.when(lat == 0)(clear_low)
        pl.when(lat == 1)(clear_high)

    loads[0].wait()
    for a in range(WLA):
        for o in range(WLO):
            cell = tokens_ref[a, o].astype(jnp.float32)
            row = octant_row(a, o)
            for side in range(WLV):
                own[o // HALF_LO, slots[side], row : row + 1, :] = cell[side : side + 1]
    loads[1].wait()
    normed = layer_norm(own[...].reshape(4 * SIDE, features), gain1_ref[...])
    for half in range(2):
        plain = normed[half * 2 * SIDE : half * 2 * SIDE + SIDE]
        paired = normed[half * 2 * SIDE + SIDE : (half + 1) * 2 * SIDE]
        tails = jnp.concatenate([plain[:, LANES:], paired[:, LANES:]], axis=1)
        for kind, block in enumerate((plain[:, :LANES], paired[:, :LANES], tails)):
            cells[1 + half, kind, PITCH : PITCH + SIDE, :] = block.astype(jnp.bfloat16)
    normed = normed.astype(jnp.bfloat16)
    pl.semaphore_wait(barrier, jnp.where(first_lon, greetings - wrapped, greetings))

    def start(*groups):
        for group in groups:
            for copy in group:
                copy.start()

    def start_side(lon_step):
        start(first_parts[lon_step], last_parts[lon_step])

    @pl.when(last_lon)
    def _():
        if sizes[1] == 2:
            for at_lat in range(2):

                @pl.when(lat == at_lat)
                def _(at_lat=at_lat):
                    for to_lat in range(2):
                        first_parts[1][at_lat ^ to_lat].start()
                        last_parts[1][at_lat ^ to_lat].start()
        else:
            start_side(1)
        tell(ready, peers[1])
        start_side(-1)

    pl.when(first_lon)(lambda: start_side(1))

    @pl.when(jnp.logical_not(first_lon | last_lon))
    def _():
        start(first_parts[1], first_parts[-1], last_parts[1], last_parts[-1])

    start(row_copies)

    loads[2].wait()
    tables[...] = jnp.zeros_like(tables)
    for head in range(HEADS):
        pair = table_ref[0, head].astype(jnp.float32)
        for kind in range(WLV):
            tables[kind, head : head + 1, :] = pair[kind : kind + 1]

    def section(kind, query_lev, key_lev, side):
        at = (query_lev * WLV + key_lev) * WLA * CHUNK + side * SECTION
        return tables[kind, :, at : at + SECTION]

    def sections(side):
        found = [
            jnp.where(lev == 0, section(kind, *low, side), section(kind, *high, side))
            for kind, low, high in ((1, (1, 1), (0, 0)), (0, (0, 0), (1, 1)), (0, (0, 1), (1, 0)))
        ]
        return jnp.concatenate(found, axis=0)

    chunks_out[...] = sections(1).astype(jnp.bfloat16)
    table_copy.start()
    own_chunks = sections(0)

    lane = lax.broadcasted_iota(jnp.int32, (ROWS, LANES), 1)
    lat_side = lane % SIDE // PITCH
    real = (lane < LATS) & (lane % PITCH < OCT)
    partner_out = (lat == 0, lat == sizes[1] - 1)

    def fill_bias(half, found):
        chunk_rows = jnp.concatenate(
            [found[:, step * CHUNK : (step + 1) * CHUNK] for step in range(HALF_LA)], axis=0
        )
        spread = matmul(chunk_rows.astype(jnp.bfloat16), pick_ref[...])
        allowed = real & ((lat_side != half) | jnp.logical_not(partner_out[half]))
        for step in range(HALF_LA):
            for kind in range(3):
                at = (step * 3 + kind) * ROWS
                for o in range(WLO):
                    tile = spread[at : at + ROWS, o * LANES : (o + 1) * LANES]
                    tile = jnp.where(allowed, tile, -1e30)
                    bias[
                        1 - o // HALF_LO,
                        half,
                        kind,
                        pl.ds(step * HALF_LO + o % HALF_LO, HEADS, stride=PITCH),
                        :,
                    ] = tile[:HEADS]

    loads[3].wait()
    fill_bias(1, own_chunks)

    loads[4].wait()
    for part in range(2):
        weight = qkv_ref[:, (part + 1) * features : (part + 2) * features]
        blank_rows = jnp.zeros((features - LANES, features), jnp.bfloat16)
        for slot in range(2):
            weights[part, slot, :LANES] = weight[:LANES]
            pieces = (weight[LANES:], blank_rows)
            for place in range(2):
                at = LANES + place * (features - LANES)
                weights[part, slot, at : at + features - LANES] = pieces[place ^ slot]
    queries = matmul(normed, qkv_ref[:, :features])
    head_of = lax.broadcasted_iota(jnp.int32, (PITCH, features), 1) // (features // HEADS)
    for octant in range(8):
        rows = queries[octant * PITCH : (octant + 1) * PITCH]
        stacked[octant // 4, octant % 4] = jnp.concatenate(
            [jnp.where(head_of == head, rows, 0.0) for head in range(HEADS)], axis=0
        ).astype(jnp.bfloat16)

    def project(column):
        plain = jnp.concatenate([cells[column, 0], cells[column, 2]], axis=1)
        paired = jnp.concatenate(
            [
                jnp.concatenate([cells[column, 1], cells[column, 2]], axis=1),
                jnp.concatenate([cells[column, 3], cells[column, 4]], axis=1),
            ],
            axis=0,
        )
        for part, kept in enumerate((keys, values)):
            kept[column, :LATS] = matmul(plain, weights[part, 0]).astype(jnp.bfloat16)
            kept[column, LATS:] = matmul(paired, weights[part, 1]).astype(jnp.bfloat16)

    def receive(phase, part):
        for at, (_, lat_from, lat_to, rows) in enumerate(moves):
            kinds = (tail_kinds, plain_kind)[part]
            remote(
                cells.at[1:2, kinds, pl.ds(lat_from, rows), :],
                cells.at[pl.ds(3 * phase, 1), kinds, pl.ds(lat_to, rows), :],
                phase * per_side + at * 2 + part,
                partner,
            ).wait_recv()

    def relay(phase):
        receive(phase, 0)
        pass_on(pl.ds(3 * phase, 1), phase).start()

    def gather(phase):
        receive(phase, 1)
        pass_on(pl.ds(3 * phase, 1), phase).wait_recv()
        project(3 * phase)

    at_wrap = first_lon | last_lon
    near = jnp.where(last_lon, 0, 1)
    for copy in row_copies:
        copy.wait_recv()
    own_pass.start()
    relay(near)
    pl.when(jnp.logical_not(at_wrap))(lambda: relay(1 - near))
    table_copy.wait_recv()
    fill_bias(0, chunks_in[...].astype(jnp.float32))
    own_pass.wait_recv()
    for column in (1, 2):
        project(column)
    for load in loads[5:]:
        load.wait()

    scale = (features // HEADS) ** (-0.5)
    rest = jnp.zeros((LANES - LATS, features), jnp.bfloat16)

    def window_rows(held_rows, phase, slot, half):
        at = slot * LATS + half * SIDE
        pieces = [held_rows[2 * phase + side, at : at + SIDE, :] for side in range(2)]
        return pieces + [rest]

    def attend(phases):
        octants = [(p, slot, half) for p in phases for slot in range(2) for half in range(2)]
        slot_keys = ((0,), (1, 2))

        def window(held_rows, phase, slot, half):
            return jnp.concatenate(
                [r for s in slot_keys[slot] for r in window_rows(held_rows, phase, s, half)], axis=0
            )

        scores = [
            lax.dot_general(
                stacked[phase, slot * 2 + half],
                window(keys, phase, slot, half),
                (((1,), (1,)), ((), ())),
                preferred_element_type=jnp.float32,
            )
            for phase, slot, half in octants
        ]
        shares, totals = [], []
        for (phase, slot, half), products in zip(octants, scores):
            added = jnp.concatenate([bias[phase, half, s] for s in slot_keys[slot]], axis=1)
            products = products * scale + added
            weight = jnp.exp(products - jnp.max(products, axis=-1, keepdims=True))
            shares.append(weight.astype(jnp.bfloat16))
            totals.append(jnp.sum(weight, axis=-1, keepdims=True))
        mixes = [
            matmul(weight, window(values, phase, slot, half))
            for (phase, slot, half), weight in zip(octants, shares)
        ]
        found = []
        for mixed, total in zip(mixes, totals):
            mixed = mixed * (1.0 / total)
            found.append(
                sum(
                    jnp.where(head_of == head, mixed[head * PITCH : (head + 1) * PITCH], 0.0)
                    for head in range(HEADS)
                )
            )
        context = jnp.concatenate(found, axis=0).astype(jnp.bfloat16)
        tokens = jnp.concatenate([own[p].reshape(4 * PITCH, features) for p in phases], axis=0)
        first = tokens + matmul(context, proj_ref[...])
        normed_two = layer_norm(first, gain2_ref[...]).astype(jnp.bfloat16)
        hidden = matmul(normed_two, fc1_ref[...])
        hidden = 0.5 * hidden * (1.0 + lax.erf(hidden * np.float32(0.5**0.5)))
        blended = first + lax.dot_general(
            hidden.astype(jnp.bfloat16),
            fc2_ref[...],
            (((1,), (1,)), ((), ())),
            preferred_element_type=jnp.float32,
        )
        for place, phase in enumerate(phases):
            at = place * 2 * SIDE
            rows_out[place] = blended[at : at + 2 * SIDE].reshape(2, SIDE, features)
            for a in range(WLA):
                for o in range(HALF_LO):
                    row = octant_row(a, o)
                    out_ref[a, phase * HALF_LO + o] = jnp.concatenate(
                        [rows_out[place, slot, row : row + 1, :] for slot in slots], axis=0
                    ).astype(jnp.bfloat16)

    @pl.when(first_lon)
    def _():
        pl.semaphore_wait(ready, wrapped)
        start_side(-1)

    def run_phase(step, _):
        phase = jnp.where(step == 0, near, 1 - near)
        pl.when(step == 1)(lambda: relay(phase))
        gather(phase)
        attend((phase,))
        return 0

    @pl.when(at_wrap)
    def _():
        lax.fori_loop(0, 2, run_phase, 0)

    @pl.when(jnp.logical_not(at_wrap))
    def _():
        gather(1)
        gather(0)
        attend((0, 1))

    for lon_step in (1, -1):
        for copy in first_parts[lon_step] + last_parts[lon_step]:
            copy.wait_send()
    for copy in row_copies + [own_pass, table_copy]:
        copy.wait_send()
    for phase in range(2):
        pass_on(slice(3 * phase, 3 * phase + 1), phase).wait_send()


def per_device(
    sizes,
    tokens,
    norm1_gain,
    qkv_weight,
    proj_weight,
    earth_bias,
    norm2_gain,
    fc1_weight,
    fc2_weight,
):
    assert tokens.shape[:3] == (WLV, WLA, WLO)
    assert sizes[0] == 2 and earth_bias.shape[0] == 2
    features = tokens.shape[-1]
    assert LANES + LANES // 2 == features
    operands = (
        tokens.transpose(1, 2, 0, 3),
        norm1_gain.reshape(1, -1),
        earth_bias.transpose(1, 2, 0, 3),
        jnp.asarray(toeplitz_matrix(), jnp.bfloat16),
        qkv_weight,
        proj_weight,
        norm2_gain.reshape(1, -1),
        fc1_weight,
        fc2_weight.T,
    )
    assert len(operands) == OPERANDS
    blended = pl.pallas_call(
        functools.partial(kernel, sizes),
        out_shape=jax.ShapeDtypeStruct(operands[0].shape, jnp.bfloat16),
        in_specs=[pl.BlockSpec(memory_space=pltpu.HBM)] * OPERANDS,
        out_specs=pl.BlockSpec(memory_space=pltpu.VMEM),
        scratch_shapes=[
            *[pltpu.VMEM(operand.shape, operand.dtype) for operand in operands],
            pltpu.VMEM((2, 2, SIDE, features), jnp.float32),
            pltpu.VMEM((4, KINDS, LATS, LANES), jnp.bfloat16),
            pltpu.VMEM((WLV, ROWS, earth_bias.shape[-1]), jnp.float32),
            pltpu.VMEM((3 * ROWS, SECTION), jnp.bfloat16),
            pltpu.VMEM((3 * ROWS, SECTION), jnp.bfloat16),
            pltpu.VMEM((2, 2, 3, STACK, LANES), jnp.float32),
            pltpu.VMEM((2, 2, 2 * LANES, features), jnp.bfloat16),
            pltpu.VMEM((2, 4, STACK, features), jnp.bfloat16),
            pltpu.VMEM((4, 3 * LATS, features), jnp.bfloat16),
            pltpu.VMEM((4, 3 * LATS, features), jnp.bfloat16),
            pltpu.VMEM((2, 2, SIDE, features), jnp.float32),
            pltpu.SemaphoreType.DMA((2, message_count(sizes))),
            pltpu.SemaphoreType.DMA((OPERANDS,)),
            pltpu.SemaphoreType.REGULAR,
        ],
        compiler_params=pltpu.CompilerParams(
            collective_id=0, has_side_effects=True, vmem_limit_bytes=48 * 1024 * 1024
        ),
    )(*[pltpu.with_memory_space_constraint(x, pltpu.HBM) for x in operands])
    return blended.transpose(2, 0, 1, 3)


def solution(mesh):
    placed = (
        P("lev", "lat", "lon", None),
        P(),
        P(),
        P(),
        P(None, "lat", None, None),
        P(),
        P(),
        P(),
    )
    return jax.shard_map(
        functools.partial(per_device, tuple(mesh.shape[axis] for axis in AXES)),
        mesh=mesh,
        in_specs=placed,
        out_specs=P("lev", "lat", "lon", None),
        check_vma=False,
    )
```

```python
import functools

import jax
import jax.numpy as jnp
import numpy as np
from jax import lax
from jax.experimental import pallas as pl
from jax.experimental.pallas import tpu as pltpu
from jax.sharding import PartitionSpec as P

HEADS = 6
WLV = 2
WLA = 6
WLO = 12
HALF_LA = WLA // 2
HALF_LO = WLO // 2
OCT = HALF_LA * HALF_LO
PITCH = 24
SIDE = 2 * PITCH
LATS = 2 * SIDE
SPAN = 2 * WLO - 1
CHUNK = WLA * SPAN
ROWS = 8
LANES = 128
AXES = ("lev", "lat", "lon")
OPERANDS = 9
STACK = HEADS * PITCH
SECTION = HALF_LA * CHUNK
KINDS = 5

norm_eps = 1e-05


def octant_row(lat, lon):
    return lat // HALF_LA * PITCH + lat % HALF_LA * HALF_LO + lon % HALF_LO


def toeplitz_matrix():
    pick = np.zeros((CHUNK, WLO * LANES), np.float32)
    for lon in range(WLO):
        for key_lat in range(WLA):
            for key_lon in range(WLO):
                column = lon * LANES + key_lon // HALF_LO * SIDE + octant_row(key_lat, key_lon)
                pick[key_lat * SPAN + lon - key_lon + WLO - 1, column] = 1
    return pick


def layer_norm(values, scale_gain):
    average = jnp.mean(values, axis=-1, keepdims=True)
    centered = values - average
    variance = jnp.mean(centered * centered, axis=-1, keepdims=True)
    return centered * lax.rsqrt(variance + norm_eps) * scale_gain


def matmul(a, b):
    return jnp.dot(a, b, preferred_element_type=jnp.float32)


def lat_moves(size, at):
    stay = (0, 1, 1, 2)
    if size == 2:
        return (stay, (1, 2 - at, 3 * at, 1))
    return (stay, (1, 2, 0, 1), (-1, 1, 3, 1))


def lon_moves():
    return (
        (1, slice(2, 3), slice(0, 1)),
        (-1, slice(1, 2), slice(3, 4)),
        (0, slice(1, 3), slice(1, 3)),
    )


def message_count(sizes):
    lats = len(lat_moves(sizes[1], 0))
    return 4 * lats + (lats - 1) + 3 + 1 + lats


def kernel(sizes, *refs):
    operands, out_ref, held = refs[:OPERANDS], refs[OPERANDS], refs[OPERANDS + 1 : -14]
    (
        own,
        cells,
        tables,
        chunks_out,
        chunks_in,
        bias,
        weights,
        stacked,
        keys,
        values,
        rows_out,
        sems,
        load_sems,
        ready,
    ) = refs[-14:]
    loads = [
        pltpu.make_async_copy(source, place, load_sems.at[i])
        for i, (source, place) in enumerate(zip(operands, held))
    ]
    for load in loads:
        load.start()
    (
        tokens_ref,
        gain1_ref,
        table_ref,
        pick_ref,
        qkv_ref,
        proj_ref,
        gain2_ref,
        fc1_ref,
        fc2_ref,
    ) = held
    lev, lat, lon = where = [lax.axis_index(axis) for axis in AXES]
    features = own.shape[-1]
    slots = (lev, 1 - lev)

    def device(steps):
        return {
            axis: lax.rem(at + step + size, size)
            for axis, at, step, size in zip(AXES, where, steps, sizes)
        }

    moves = lat_moves(sizes[1], lat)
    per_side = 2 * len(moves)

    def remote(source, target, index, there):
        return pltpu.make_async_remote_copy(
            src_ref=source,
            dst_ref=target,
            send_sem=sems.at[0, index],
            recv_sem=sems.at[1, index],
            device_id=there,
            device_id_type=pl.DeviceIdType.MESH,
        )

    def part_of(columns, kinds, octants):
        return cells.at[columns, kinds, octants, 0:OCT, :]

    tail_kinds, plain_kind, passed_kinds = slice(1, 3), slice(0, 1), slice(3, 5)
    first_parts, last_parts, peers = {}, {}, {}
    for side, (lon_step, lon_from, lon_to) in enumerate(lon_moves()[:2]):
        first_parts[lon_step], last_parts[lon_step], peers[lon_step] = [], [], []
        for at, (lat_step, lat_from, lat_to, octants) in enumerate(moves):
            there = device((0, lat_step, lon_step))
            peers[lon_step].append(there)
            for part, kinds in enumerate((tail_kinds, plain_kind)):
                (first_parts, last_parts)[part][lon_step].append(
                    remote(
                        part_of(lon_from, kinds, pl.ds(lat_from, octants)),
                        part_of(lon_to, kinds, pl.ds(lat_to, octants)),
                        side * per_side + at * 2 + part,
                        there,
                    )
                )
    row_copies, row_peers = [], []
    for at, (lat_step, lat_from, lat_to, octants) in enumerate(moves[1:]):
        row_peers.append(device((0, lat_step, 0)))
        row_copies.append(
            remote(
                part_of(slice(1, 3), slice(0, 3), pl.ds(lat_from, octants)),
                part_of(slice(1, 3), slice(0, 3), pl.ds(lat_to, octants)),
                2 * per_side + at,
                row_peers[-1],
            )
        )
    partner = device((1, 0, 0))
    passed = 2 * per_side + len(row_copies)
    used = pl.ds(1 - lat, 3) if sizes[1] == 2 else slice(0, 4)

    def pass_on(columns, index):
        return remote(
            part_of(columns, tail_kinds, used),
            part_of(columns, passed_kinds, used),
            passed + index,
            partner,
        )

    own_pass = pass_on(slice(1, 3), 2)
    table_copy = remote(chunks_out, chunks_in, passed + 3, device((0, 1, 0)))
    crossings, cross_peers = {}, {}
    for lon_step, lon_from, lon_to in lon_moves()[:2]:
        crossings[lon_step], cross_peers[lon_step] = [], []
        for at, (lat_step, lat_from, lat_to, octants) in enumerate(moves):
            there = device((1, lat_step, lon_step))
            cross_peers[lon_step].append(there)
            crossings[lon_step].append(
                remote(
                    part_of(lon_from, tail_kinds, pl.ds(lat_from, octants)),
                    part_of(lon_to, passed_kinds, pl.ds(lat_to, octants)),
                    passed + 4 + at,
                    there,
                )
            )

    barrier = pltpu.get_barrier_semaphore()
    first_lon, last_lon = lon == 0, lon == sizes[2] - 1
    before_last = lon == sizes[2] - 2
    at_wrap = first_lon | last_lon

    def tell(semaphore, group):
        for there in group:
            pl.semaphore_signal(
                semaphore, inc=1, device_id=there, device_id_type=pl.DeviceIdType.MESH
            )

    def start(*groups):
        for group in groups:
            for copy in group:
                copy.start()

    wrapped = len(moves)
    greetings = len(row_peers) + 1 + 2 * wrapped
    tell(barrier, peers[-1])
    pl.when(first_lon)(lambda: tell(barrier, cross_peers[-1]))
    pl.when(last_lon)(lambda: tell(barrier, [device((1, 0, -1))]))
    pl.when(jnp.logical_not(last_lon))(lambda: tell(barrier, row_peers + [partner]))
    pl.when(jnp.logical_not(last_lon | before_last))(lambda: tell(barrier, peers[1]))

    cells[:, :, :, OCT:, :] = jnp.zeros((4, KINDS, 4, PITCH - OCT, LANES), jnp.bfloat16)
    for pad in (OCT, PITCH + OCT):
        own[:, :, pad : pad + PITCH - OCT, :] = jnp.zeros(
            (2, 2, PITCH - OCT, features), jnp.float32
        )
    if sizes[1] == 2:
        blank = jnp.zeros((4, KINDS, PITCH, LANES), jnp.bfloat16)

        def clear_low():
            cells[:, :, 0] = blank

        def clear_high():
            cells[:, :, 3] = blank

        pl.when(lat == 0)(clear_low)
        pl.when(lat == 1)(clear_high)

    @pl.when(last_lon)
    def _():
        pl.semaphore_wait(barrier, 2 * wrapped)
        tell(ready, peers[1] + cross_peers[1])

    loads[0].wait()
    for a in range(WLA):
        for o in range(WLO):
            cell = tokens_ref[a, o].astype(jnp.float32)
            row = octant_row(a, o)
            for side in range(WLV):
                own[o // HALF_LO, slots[side], row : row + 1, :] = cell[side : side + 1]
    loads[1].wait()
    normed = layer_norm(own[...].reshape(4 * SIDE, features), gain1_ref[...])
    for half in range(2):
        plain = normed[half * 2 * SIDE : half * 2 * SIDE + SIDE]
        paired = normed[half * 2 * SIDE + SIDE : (half + 1) * 2 * SIDE]
        tails = jnp.concatenate([plain[:, LANES:], paired[:, LANES:]], axis=1)
        for kind, block in enumerate((plain[:, :LANES], paired[:, :LANES], tails)):
            cells[1 + half, kind, 1:3] = block.reshape(2, PITCH, LANES).astype(jnp.bfloat16)
    normed = normed.astype(jnp.bfloat16)

    def over_wrap(lon_step, at_lat, at_lev):
        own = [first_parts[lon_step], last_parts[lon_step]]
        for to_lat in range(2):
            index = at_lat ^ to_lat
            groups = [own, [crossings[lon_step]]]
            for group in groups[at_lev], groups[1 - at_lev]:
                for copies in group:
                    copies[index].start()

    def send_over_wrap(lon_step, order):
        if sizes[1] != 2:
            start(first_parts[lon_step], last_parts[lon_step], crossings[lon_step])
            return
        for at_lat in range(2):
            for at_lev in range(2):
                pl.when((lat == at_lat) & (lev == at_lev))(
                    functools.partial(over_wrap, lon_step, at_lat, at_lev ^ order)
                )

    pl.when(last_lon)(lambda: send_over_wrap(1, 0))

    @pl.when(jnp.logical_not(last_lon))
    def _():
        expected = jnp.where(first_lon, greetings - wrapped, greetings)
        pl.semaphore_wait(barrier, jnp.where(before_last, greetings + 1, expected))
        pl.when(before_last)(lambda: tell(ready, peers[1]))
        pl.when(jnp.logical_not(first_lon))(lambda: start(first_parts[-1], last_parts[-1]))
        start(row_copies, first_parts[1], last_parts[1])

    loads[2].wait()
    tables[...] = jnp.zeros_like(tables)
    for head in range(HEADS):
        pair = table_ref[0, head].astype(jnp.float32)
        for kind in range(WLV):
            tables[kind, head : head + 1, :] = pair[kind : kind + 1]

    def section(kind, query_lev, key_lev, side):
        at = (query_lev * WLV + key_lev) * WLA * CHUNK + side * SECTION
        return tables[kind, :, at : at + SECTION]

    def sections(side):
        found = [
            jnp.where(lev == 0, section(kind, *low, side), section(kind, *high, side))
            for kind, low, high in ((1, (1, 1), (0, 0)), (0, (0, 0), (1, 1)), (0, (0, 1), (1, 0)))
        ]
        return jnp.concatenate(found, axis=0)

    chunks_out[...] = sections(1).astype(jnp.bfloat16)
    pl.when(jnp.logical_not(last_lon))(table_copy.start)
    own_chunks = sections(0)

    lane = lax.broadcasted_iota(jnp.int32, (ROWS, LANES), 1)
    lat_side = lane % SIDE // PITCH
    real = (lane < LATS) & (lane % PITCH < OCT)
    partner_out = (lat == 0, lat == sizes[1] - 1)

    def fill_bias(half, found):
        chunk_rows = jnp.concatenate(
            [found[:, step * CHUNK : (step + 1) * CHUNK] for step in range(HALF_LA)], axis=0
        )
        spread = matmul(chunk_rows.astype(jnp.bfloat16), pick_ref[...])
        allowed = real & ((lat_side != half) | jnp.logical_not(partner_out[half]))
        for step in range(HALF_LA):
            for kind in range(3):
                at = (step * 3 + kind) * ROWS
                for o in range(WLO):
                    tile = spread[at : at + ROWS, o * LANES : (o + 1) * LANES]
                    tile = jnp.where(allowed, tile, -1e30)
                    bias[
                        1 - o // HALF_LO,
                        half,
                        kind,
                        pl.ds(step * HALF_LO + o % HALF_LO, HEADS, stride=PITCH),
                        :,
                    ] = tile[:HEADS]

    loads[3].wait()
    fill_bias(1, own_chunks)

    loads[4].wait()
    for part in range(2):
        weight = qkv_ref[:, (part + 1) * features : (part + 2) * features]
        blank_rows = jnp.zeros((features - LANES, features), jnp.bfloat16)
        for slot in range(2):
            weights[part, slot, :LANES] = weight[:LANES]
            pieces = (weight[LANES:], blank_rows)
            for place in range(2):
                at = LANES + place * (features - LANES)
                weights[part, slot, at : at + features - LANES] = pieces[place ^ slot]
    queries = matmul(normed, qkv_ref[:, :features])
    head_of = lax.broadcasted_iota(jnp.int32, (PITCH, features), 1) // (features // HEADS)
    for octant in range(8):
        rows = queries[octant * PITCH : (octant + 1) * PITCH]
        stacked[octant // 4, octant % 4] = jnp.concatenate(
            [jnp.where(head_of == head, rows, 0.0) for head in range(HEADS)], axis=0
        ).astype(jnp.bfloat16)

    def project(column):
        plain, paired, tails, passed_on, passed_tails = (
            cells[column, kind].reshape(LATS, LANES) for kind in range(KINDS)
        )
        plain = jnp.concatenate([plain, tails], axis=1)
        paired = jnp.concatenate(
            [
                jnp.concatenate([paired, tails], axis=1),
                jnp.concatenate([passed_on, passed_tails], axis=1),
            ],
            axis=0,
        )
        for part, kept in enumerate((keys, values)):
            kept[column, :LATS] = matmul(plain, weights[part, 0]).astype(jnp.bfloat16)
            kept[column, LATS:] = matmul(paired, weights[part, 1]).astype(jnp.bfloat16)

    def receive(phase, part):
        for at, (_, lat_from, lat_to, octants) in enumerate(moves):
            kinds = (tail_kinds, plain_kind)[part]
            remote(
                part_of(slice(1, 2), kinds, pl.ds(lat_from, octants)),
                part_of(pl.ds(3 * phase, 1), kinds, pl.ds(lat_to, octants)),
                phase * per_side + at * 2 + part,
                partner,
            ).wait_recv()

    def relay(phase):
        receive(phase, 0)
        pass_on(pl.ds(3 * phase, 1), phase).start()

    def relayed(phase):
        pass_on(pl.ds(3 * phase, 1), phase).wait_recv()

    near = jnp.where(last_lon, 0, 1)

    @pl.when(last_lon)
    def _():
        pl.semaphore_wait(ready, wrapped)
        start(row_copies, [table_copy], first_parts[-1], last_parts[-1])

    for copy in row_copies:
        copy.wait_recv()
    own_pass.start()
    relay(near)
    pl.when(jnp.logical_not(at_wrap))(lambda: relay(1 - near))
    table_copy.wait_recv()
    fill_bias(0, chunks_in[...].astype(jnp.float32))
    own_pass.wait_recv()
    for column in (1, 2):
        project(column)
    for load in loads[5:]:
        load.wait()

    scale = (features // HEADS) ** (-0.5)
    rest = jnp.zeros((LANES - LATS, features), jnp.bfloat16)

    def window_rows(held_rows, phase, slot, half):
        at = slot * LATS + half * SIDE
        pieces = [held_rows[2 * phase + side, at : at + SIDE, :] for side in range(2)]
        return pieces + [rest]

    def attend(phases):
        octants = [(p, slot, half) for p in phases for slot in range(2) for half in range(2)]
        slot_keys = ((0,), (1, 2))

        def window(held_rows, phase, slot, half):
            return jnp.concatenate(
                [r for s in slot_keys[slot] for r in window_rows(held_rows, phase, s, half)], axis=0
            )

        scores = [
            lax.dot_general(
                stacked[phase, slot * 2 + half],
                window(keys, phase, slot, half),
                (((1,), (1,)), ((), ())),
                preferred_element_type=jnp.float32,
            )
            for phase, slot, half in octants
        ]
        shares, totals = [], []
        for (phase, slot, half), products in zip(octants, scores):
            added = jnp.concatenate([bias[phase, half, s] for s in slot_keys[slot]], axis=1)
            products = products * scale + added
            weight = jnp.exp(products - jnp.max(products, axis=-1, keepdims=True))
            shares.append(weight.astype(jnp.bfloat16))
            totals.append(jnp.sum(weight, axis=-1, keepdims=True))
        mixes = [
            matmul(weight, window(values, phase, slot, half))
            for (phase, slot, half), weight in zip(octants, shares)
        ]
        found = []
        for mixed, total in zip(mixes, totals):
            mixed = mixed * (1.0 / total)
            found.append(
                sum(
                    jnp.where(head_of == head, mixed[head * PITCH : (head + 1) * PITCH], 0.0)
                    for head in range(HEADS)
                )
            )
        context = jnp.concatenate(found, axis=0).astype(jnp.bfloat16)
        tokens = jnp.concatenate([own[p].reshape(4 * PITCH, features) for p in phases], axis=0)
        first = tokens + matmul(context, proj_ref[...])
        normed_two = layer_norm(first, gain2_ref[...]).astype(jnp.bfloat16)
        hidden = matmul(normed_two, fc1_ref[...])
        hidden = 0.5 * hidden * (1.0 + lax.erf(hidden * np.float32(0.5**0.5)))
        blended = first + lax.dot_general(
            hidden.astype(jnp.bfloat16),
            fc2_ref[...],
            (((1,), (1,)), ((), ())),
            preferred_element_type=jnp.float32,
        )
        for place, phase in enumerate(phases):
            at = place * 2 * SIDE
            rows_out[place] = blended[at : at + 2 * SIDE].reshape(2, SIDE, features)
            for a in range(WLA):
                for o in range(HALF_LO):
                    row = octant_row(a, o)
                    out_ref[a, phase * HALF_LO + o] = jnp.concatenate(
                        [rows_out[place, slot, row : row + 1, :] for slot in slots], axis=0
                    ).astype(jnp.bfloat16)

    @pl.when(first_lon)
    def _():
        pl.semaphore_wait(ready, 2 * wrapped)
        send_over_wrap(-1, 1)

    def run_phase(step, _):
        phase = jnp.where(step == 0, near, 1 - near)
        pl.when(step == 0)(lambda: relayed(phase))

        @pl.when(step == 1)
        def _():
            receive(phase, 0)
            for copy in crossings[1]:
                copy.wait_recv()

        receive(phase, 1)
        project(3 * phase)
        attend((phase,))
        return 0

    @pl.when(at_wrap)
    def _():
        lax.fori_loop(0, 2, run_phase, 0)
        pass_on(pl.ds(3 * near, 1), near).wait_send()
        for copy in crossings[1]:
            copy.wait_send()

    @pl.when(jnp.logical_not(at_wrap))
    def _():
        for phase in (1, 0):
            receive(phase, 1)
            relayed(phase)
            project(3 * phase)
        attend((0, 1))
        for phase in range(2):
            pass_on(slice(3 * phase, 3 * phase + 1), phase).wait_send()

    for lon_step in (1, -1):
        for copy in first_parts[lon_step] + last_parts[lon_step]:
            copy.wait_send()
    for copy in row_copies + [own_pass, table_copy]:
        copy.wait_send()


def per_device(
    sizes,
    tokens,
    norm1_gain,
    qkv_weight,
    proj_weight,
    earth_bias,
    norm2_gain,
    fc1_weight,
    fc2_weight,
):
    assert tokens.shape[:3] == (WLV, WLA, WLO)
    assert sizes[0] == 2 and sizes[2] > 3 and earth_bias.shape[0] == 2
    features = tokens.shape[-1]
    assert LANES + LANES // 2 == features
    operands = (
        tokens.transpose(1, 2, 0, 3),
        norm1_gain.reshape(1, -1),
        earth_bias.transpose(1, 2, 0, 3),
        jnp.asarray(toeplitz_matrix(), jnp.bfloat16),
        qkv_weight,
        proj_weight,
        norm2_gain.reshape(1, -1),
        fc1_weight,
        fc2_weight.T,
    )
    assert len(operands) == OPERANDS
    blended = pl.pallas_call(
        functools.partial(kernel, sizes),
        out_shape=jax.ShapeDtypeStruct(operands[0].shape, jnp.bfloat16),
        in_specs=[pl.BlockSpec(memory_space=pltpu.HBM)] * OPERANDS,
        out_specs=pl.BlockSpec(memory_space=pltpu.VMEM),
        scratch_shapes=[
            *[pltpu.VMEM(operand.shape, operand.dtype) for operand in operands],
            pltpu.VMEM((2, 2, SIDE, features), jnp.float32),
            pltpu.VMEM((4, KINDS, 4, PITCH, LANES), jnp.bfloat16),
            pltpu.VMEM((WLV, ROWS, earth_bias.shape[-1]), jnp.float32),
            pltpu.VMEM((3 * ROWS, SECTION), jnp.bfloat16),
            pltpu.VMEM((3 * ROWS, SECTION), jnp.bfloat16),
            pltpu.VMEM((2, 2, 3, STACK, LANES), jnp.float32),
            pltpu.VMEM((2, 2, 2 * LANES, features), jnp.bfloat16),
            pltpu.VMEM((2, 4, STACK, features), jnp.bfloat16),
            pltpu.VMEM((4, 3 * LATS, features), jnp.bfloat16),
            pltpu.VMEM((4, 3 * LATS, features), jnp.bfloat16),
            pltpu.VMEM((2, 2, SIDE, features), jnp.float32),
            pltpu.SemaphoreType.DMA((2, message_count(sizes))),
            pltpu.SemaphoreType.DMA((OPERANDS,)),
            pltpu.SemaphoreType.REGULAR,
        ],
        compiler_params=pltpu.CompilerParams(
            collective_id=0, has_side_effects=True, vmem_limit_bytes=48 * 1024 * 1024
        ),
    )(*[pltpu.with_memory_space_constraint(x, pltpu.HBM) for x in operands])
    return blended.transpose(2, 0, 1, 3)


def solution(mesh):
    placed = (
        P("lev", "lat", "lon", None),
        P(),
        P(),
        P(),
        P(None, "lat", None, None),
        P(),
        P(),
        P(),
    )
    return jax.shard_map(
        functools.partial(per_device, tuple(mesh.shape[axis] for axis in AXES)),
        mesh=mesh,
        in_specs=placed,
        out_specs=P("lev", "lat", "lon", None),
        check_vma=False,
    )
```

```python
import functools

import jax
import jax.numpy as jnp
import numpy as np
from jax import lax
from jax.experimental import pallas as pl
from jax.experimental.pallas import tpu as pltpu
from jax.sharding import PartitionSpec as P

HEADS = 6
WLV = 2
WLA = 6
WLO = 12
HALF_LA = WLA // 2
HALF_LO = WLO // 2
OCT = HALF_LA * HALF_LO
PITCH = 24
SIDE = 2 * PITCH
LATS = 2 * SIDE
SPAN = 2 * WLO - 1
CHUNK = WLA * SPAN
ROWS = 8
LANES = 128
AXES = ("lev", "lat", "lon")
OPERANDS = 9
STACK = HEADS * PITCH
SECTION = HALF_LA * CHUNK
KINDS = 5

norm_eps = 1e-05


def octant_row(lat, lon):
    return lat // HALF_LA * PITCH + lat % HALF_LA * HALF_LO + lon % HALF_LO


def toeplitz_matrix():
    pick = np.zeros((CHUNK, WLO * LANES), np.float32)
    for lon in range(WLO):
        for key_lat in range(WLA):
            for key_lon in range(WLO):
                column = lon * LANES + key_lon // HALF_LO * SIDE + octant_row(key_lat, key_lon)
                pick[key_lat * SPAN + lon - key_lon + WLO - 1, column] = 1
    return pick


def matmul(a, b):
    return jnp.dot(a, b, preferred_element_type=jnp.float32)


def lat_moves(size, at):
    stay = (0, 1, 1, 2)
    if size == 2:
        return (stay, (1, 2 - at, 3 * at, 1))
    return (stay, (1, 2, 0, 1), (-1, 1, 3, 1))


def lon_moves():
    return (
        (1, slice(2, 3), slice(0, 1)),
        (-1, slice(1, 2), slice(3, 4)),
        (0, slice(1, 3), slice(1, 3)),
    )


def message_count(sizes):
    lats = len(lat_moves(sizes[1], 0))
    return 4 * lats + (lats - 1) + 3 + 1 + lats


def kernel(sizes, *refs):
    operands, out_ref, held = refs[:OPERANDS], refs[OPERANDS], refs[OPERANDS + 1 : -15]
    (
        own,
        cells,
        tables,
        chunks_out,
        chunks_in,
        bias,
        weights,
        stacked,
        keys,
        values,
        rows_out,
        sems,
        load_sems,
        ready,
        means,
    ) = refs[-15:]
    loads = [
        pltpu.make_async_copy(source, place, load_sems.at[i])
        for i, (source, place) in enumerate(zip(operands, held))
    ]
    for load in loads:
        load.start()
    (
        tokens_ref,
        gain1_ref,
        table_ref,
        pick_ref,
        qkv_ref,
        proj_ref,
        gain2_ref,
        fc1_ref,
        fc2_ref,
    ) = held
    lev, lat, lon = where = [lax.axis_index(axis) for axis in AXES]
    features = own.shape[-1]
    slots = (lev, 1 - lev)

    def device(steps):
        return {
            axis: lax.rem(at + step + size, size)
            for axis, at, step, size in zip(AXES, where, steps, sizes)
        }

    moves = lat_moves(sizes[1], lat)
    per_side = 2 * len(moves)

    def remote(source, target, index, there):
        return pltpu.make_async_remote_copy(
            src_ref=source,
            dst_ref=target,
            send_sem=sems.at[0, index],
            recv_sem=sems.at[1, index],
            device_id=there,
            device_id_type=pl.DeviceIdType.MESH,
        )

    def part_of(columns, kinds, octants):
        return cells.at[columns, kinds, octants, 0:OCT, :]

    tail_kinds, plain_kind, passed_kinds = slice(1, 3), slice(0, 1), slice(3, 5)
    first_parts, last_parts, peers = {}, {}, {}
    for side, (lon_step, lon_from, lon_to) in enumerate(lon_moves()[:2]):
        first_parts[lon_step], last_parts[lon_step], peers[lon_step] = [], [], []
        for at, (lat_step, lat_from, lat_to, octants) in enumerate(moves):
            there = device((0, lat_step, lon_step))
            peers[lon_step].append(there)
            for part, kinds in enumerate((tail_kinds, plain_kind)):
                (first_parts, last_parts)[part][lon_step].append(
                    remote(
                        part_of(lon_from, kinds, pl.ds(lat_from, octants)),
                        part_of(lon_to, kinds, pl.ds(lat_to, octants)),
                        side * per_side + at * 2 + part,
                        there,
                    )
                )
    row_copies, row_peers = [], []
    for at, (lat_step, lat_from, lat_to, octants) in enumerate(moves[1:]):
        row_peers.append(device((0, lat_step, 0)))
        row_copies.append(
            remote(
                part_of(slice(1, 3), slice(0, 3), pl.ds(lat_from, octants)),
                part_of(slice(1, 3), slice(0, 3), pl.ds(lat_to, octants)),
                2 * per_side + at,
                row_peers[-1],
            )
        )
    partner = device((1, 0, 0))
    passed = 2 * per_side + len(row_copies)
    used = pl.ds(1 - lat, 3) if sizes[1] == 2 else slice(0, 4)

    def pass_on(columns, index):
        return remote(
            part_of(columns, tail_kinds, used),
            part_of(columns, passed_kinds, used),
            passed + index,
            partner,
        )

    own_pass = pass_on(slice(1, 3), 2)
    table_copy = remote(chunks_out, chunks_in, passed + 3, device((0, 1, 0)))
    crossings, cross_peers = {}, {}
    for lon_step, lon_from, lon_to in lon_moves()[:2]:
        crossings[lon_step], cross_peers[lon_step] = [], []
        for at, (lat_step, lat_from, lat_to, octants) in enumerate(moves):
            there = device((1, lat_step, lon_step))
            cross_peers[lon_step].append(there)
            crossings[lon_step].append(
                remote(
                    part_of(lon_from, tail_kinds, pl.ds(lat_from, octants)),
                    part_of(lon_to, passed_kinds, pl.ds(lat_to, octants)),
                    passed + 4 + at,
                    there,
                )
            )

    barrier = pltpu.get_barrier_semaphore()
    first_lon, last_lon = lon == 0, lon == sizes[2] - 1
    before_last = lon == sizes[2] - 2
    at_wrap = first_lon | last_lon

    def tell(semaphore, group):
        for there in group:
            pl.semaphore_signal(
                semaphore, inc=1, device_id=there, device_id_type=pl.DeviceIdType.MESH
            )

    def start(*groups):
        for group in groups:
            for copy in group:
                copy.start()

    wrapped = len(moves)
    greetings = len(row_peers) + 1 + 2 * wrapped
    tell(barrier, peers[-1])
    pl.when(first_lon)(lambda: tell(barrier, cross_peers[-1]))
    pl.when(last_lon)(lambda: tell(barrier, [device((1, 0, -1))]))
    pl.when(jnp.logical_not(last_lon))(lambda: tell(barrier, row_peers + [partner]))
    pl.when(jnp.logical_not(last_lon | before_last))(lambda: tell(barrier, peers[1]))

    cells[:, :, :, OCT:, :] = jnp.zeros((4, KINDS, 4, PITCH - OCT, LANES), jnp.bfloat16)
    for pad in (OCT, PITCH + OCT):
        own[:, :, pad : pad + PITCH - OCT, :] = jnp.zeros(
            (2, 2, PITCH - OCT, features), jnp.float32
        )
    if sizes[1] == 2:
        blank = jnp.zeros((4, KINDS, PITCH, LANES), jnp.bfloat16)

        def clear_low():
            cells[:, :, 0] = blank

        def clear_high():
            cells[:, :, 3] = blank

        pl.when(lat == 0)(clear_low)
        pl.when(lat == 1)(clear_high)

    @pl.when(last_lon)
    def _():
        pl.semaphore_wait(barrier, 2 * wrapped)
        tell(ready, peers[1] + cross_peers[1])

    loads[0].wait()
    for a in range(WLA):
        for o in range(WLO):
            cell = tokens_ref[a, o].astype(jnp.float32)
            row = octant_row(a, o)
            for side in range(WLV):
                own[o // HALF_LO, slots[side], row : row + 1, :] = cell[side : side + 1]
    loads[1].wait()
    raw = own[...].reshape(4 * SIDE, features)
    averages = jnp.mean(raw, axis=-1, keepdims=True)
    normed = raw - averages
    scales = lax.rsqrt(jnp.mean(normed * normed, axis=-1, keepdims=True) + norm_eps)
    normed = normed * scales * gain1_ref[...]
    lower = lax.broadcasted_iota(jnp.int32, (SIDE, LANES), 1) < features - LANES
    tail_gain = jnp.concatenate([gain1_ref[:, LANES:]] * 2, axis=1)
    for half in range(2):
        pair = [slice(at, at + SIDE) for at in (half * 2 * SIDE, (half * 2 + 1) * SIDE)]
        tails = jnp.concatenate([raw[rows, LANES:] for rows in pair], axis=1)
        average, by = (
            jnp.where(lower, found[pair[0]], found[pair[1]]) for found in (averages, scales)
        )
        tails = (tails - average) * by * tail_gain
        for kind, block in enumerate((normed[pair[0], :LANES], normed[pair[1], :LANES], tails)):
            cells[1 + half, kind, 1:3] = block.reshape(2, PITCH, LANES).astype(jnp.bfloat16)
    normed = normed.astype(jnp.bfloat16)

    def over_wrap(lon_step, at_lat, at_lev):
        own = [first_parts[lon_step], last_parts[lon_step]]
        for to_lat in range(2):
            index = at_lat ^ to_lat
            groups = [own, [crossings[lon_step]]]
            for group in groups[at_lev], groups[1 - at_lev]:
                for copies in group:
                    copies[index].start()

    def send_over_wrap(lon_step, order):
        if sizes[1] != 2:
            start(first_parts[lon_step], last_parts[lon_step], crossings[lon_step])
            return
        for at_lat in range(2):
            for at_lev in range(2):
                pl.when((lat == at_lat) & (lev == at_lev))(
                    functools.partial(over_wrap, lon_step, at_lat, at_lev ^ order)
                )

    pl.when(last_lon)(lambda: send_over_wrap(1, 0))

    @pl.when(jnp.logical_not(last_lon))
    def _():
        expected = jnp.where(first_lon, greetings - wrapped, greetings)
        pl.semaphore_wait(barrier, jnp.where(before_last, greetings + 1, expected))
        pl.when(before_last)(lambda: tell(ready, peers[1]))
        pl.when(jnp.logical_not(first_lon))(lambda: start(first_parts[-1], last_parts[-1]))
        start(row_copies, first_parts[1], last_parts[1])

    loads[2].wait()
    tables[...] = jnp.zeros_like(tables)
    for head in range(HEADS):
        pair = table_ref[0, head].astype(jnp.float32)
        for kind in range(WLV):
            tables[kind, head : head + 1, :] = pair[kind : kind + 1]

    def section(kind, query_lev, key_lev, side):
        at = (query_lev * WLV + key_lev) * WLA * CHUNK + side * SECTION
        return tables[kind, :, at : at + SECTION]

    def sections(side):
        found = [
            jnp.where(lev == 0, section(kind, *low, side), section(kind, *high, side))
            for kind, low, high in ((1, (1, 1), (0, 0)), (0, (0, 0), (1, 1)), (0, (0, 1), (1, 0)))
        ]
        return jnp.concatenate(found, axis=0)

    chunks_out[...] = sections(1).astype(jnp.bfloat16)
    pl.when(jnp.logical_not(last_lon))(table_copy.start)
    own_chunks = sections(0)

    lane = lax.broadcasted_iota(jnp.int32, (ROWS, LANES), 1)
    lat_side = lane % SIDE // PITCH
    real = (lane < LATS) & (lane % PITCH < OCT)
    partner_out = (lat == 0, lat == sizes[1] - 1)

    def fill_bias(half, found):
        chunk_rows = jnp.concatenate(
            [found[:, step * CHUNK : (step + 1) * CHUNK] for step in range(HALF_LA)], axis=0
        )
        spread = matmul(chunk_rows.astype(jnp.bfloat16), pick_ref[...])
        allowed = real & ((lat_side != half) | jnp.logical_not(partner_out[half]))
        for step in range(HALF_LA):
            for kind in range(3):
                at = (step * 3 + kind) * ROWS
                for o in range(WLO):
                    tile = spread[at : at + ROWS, o * LANES : (o + 1) * LANES]
                    tile = jnp.where(allowed, tile, -1e30)
                    bias[
                        1 - o // HALF_LO,
                        half,
                        kind,
                        pl.ds(step * HALF_LO + o % HALF_LO, HEADS, stride=PITCH),
                        :,
                    ] = tile[:HEADS]

    loads[3].wait()
    fill_bias(1, own_chunks)

    loads[4].wait()
    for part in range(2):
        weight = qkv_ref[:, (part + 1) * features : (part + 2) * features]
        blank_rows = jnp.zeros((features - LANES, features), jnp.bfloat16)
        for slot in range(2):
            weights[part, slot, :LANES] = weight[:LANES]
            pieces = (weight[LANES:], blank_rows)
            for place in range(2):
                at = LANES + place * (features - LANES)
                weights[part, slot, at : at + features - LANES] = pieces[place ^ slot]
    queries = matmul(normed, qkv_ref[:, :features])
    head_of = lax.broadcasted_iota(jnp.int32, (PITCH, features), 1) // (features // HEADS)
    for octant in range(8):
        rows = queries[octant * PITCH : (octant + 1) * PITCH]
        stacked[octant // 4, octant % 4] = jnp.concatenate(
            [jnp.where(head_of == head, rows, 0.0) for head in range(HEADS)], axis=0
        ).astype(jnp.bfloat16)

    def project(column):
        plain, paired, tails, passed_on, passed_tails = (
            cells[column, kind].reshape(LATS, LANES) for kind in range(KINDS)
        )
        plain = jnp.concatenate([plain, tails], axis=1)
        paired = jnp.concatenate(
            [
                jnp.concatenate([paired, tails], axis=1),
                jnp.concatenate([passed_on, passed_tails], axis=1),
            ],
            axis=0,
        )
        for part, kept in enumerate((keys, values)):
            kept[column, :LATS] = matmul(plain, weights[part, 0]).astype(jnp.bfloat16)
            kept[column, LATS:] = matmul(paired, weights[part, 1]).astype(jnp.bfloat16)

    def receive(phase, part):
        for at, (_, lat_from, lat_to, octants) in enumerate(moves):
            kinds = (tail_kinds, plain_kind)[part]
            remote(
                part_of(slice(1, 2), kinds, pl.ds(lat_from, octants)),
                part_of(pl.ds(3 * phase, 1), kinds, pl.ds(lat_to, octants)),
                phase * per_side + at * 2 + part,
                partner,
            ).wait_recv()

    def relay(phase):
        receive(phase, 0)
        pass_on(pl.ds(3 * phase, 1), phase).start()

    def relayed(phase):
        pass_on(pl.ds(3 * phase, 1), phase).wait_recv()

    near = jnp.where(last_lon, 0, 1)

    @pl.when(last_lon)
    def _():
        pl.semaphore_wait(ready, wrapped)
        start(row_copies, [table_copy], first_parts[-1], last_parts[-1])

    for copy in row_copies:
        copy.wait_recv()
    own_pass.start()
    @pl.when(first_lon)
    def _():
        pl.semaphore_wait(ready, 2 * wrapped)
        send_over_wrap(-1, 1)

    relay(near)
    pl.when(jnp.logical_not(at_wrap))(lambda: relay(1 - near))
    table_copy.wait_recv()
    fill_bias(0, chunks_in[...].astype(jnp.float32))
    own_pass.wait_recv()
    for column in (1, 2):
        project(column)
    for load in loads[5:]:
        load.wait()
    row_mean = jnp.mean(proj_ref[...].astype(jnp.float32), axis=-1, keepdims=True)
    high_part = row_mean.astype(jnp.bfloat16)
    low_part = (row_mean - high_part.astype(jnp.float32)).astype(jnp.bfloat16)
    for part, column in enumerate((high_part, low_part)):
        means[:, part * LANES : (part + 1) * LANES] = jnp.broadcast_to(column, (features, LANES))

    scale = (features // HEADS) ** (-0.5)
    rest = jnp.zeros((LANES - LATS, features), jnp.bfloat16)

    def window_rows(held_rows, phase, slot, half):
        at = slot * LATS + half * SIDE
        pieces = [held_rows[2 * phase + side, at : at + SIDE, :] for side in range(2)]
        return pieces + [rest]

    def attend(phases):
        octants = [(p, slot, half) for p in phases for slot in range(2) for half in range(2)]
        slot_keys = ((0,), (1, 2))

        def window(held_rows, phase, slot, half):
            return jnp.concatenate(
                [r for s in slot_keys[slot] for r in window_rows(held_rows, phase, s, half)], axis=0
            )

        scores = [
            lax.dot_general(
                stacked[phase, slot * 2 + half],
                window(keys, phase, slot, half),
                (((1,), (1,)), ((), ())),
                preferred_element_type=jnp.float32,
            )
            for phase, slot, half in octants
        ]
        shares, totals = [], []
        for (phase, slot, half), products in zip(octants, scores):
            added = jnp.concatenate([bias[phase, half, s] for s in slot_keys[slot]], axis=1)
            products = products * scale + added
            weight = jnp.exp(products - jnp.max(products, axis=-1, keepdims=True))
            shares.append(weight.astype(jnp.bfloat16))
            totals.append(jnp.sum(weight, axis=-1, keepdims=True))
        mixes = [
            matmul(weight, window(values, phase, slot, half))
            for (phase, slot, half), weight in zip(octants, shares)
        ]
        found = []
        for mixed, total in zip(mixes, totals):
            mixed = mixed * (1.0 / total)
            found.append(
                sum(
                    jnp.where(head_of == head, mixed[head * PITCH : (head + 1) * PITCH], 0.0)
                    for head in range(HEADS)
                )
            )
        context = jnp.concatenate(found, axis=0).astype(jnp.bfloat16)
        tokens = jnp.concatenate([own[p].reshape(4 * PITCH, features) for p in phases], axis=0)
        average = matmul(context, means[...])
        average = average[:, :LANES] + average[:, LANES:]
        average = average + jnp.mean(tokens, axis=-1, keepdims=True)
        first = tokens + matmul(context, proj_ref[...])
        centered = first - jnp.concatenate([average, average[:, : features - LANES]], axis=1)
        variance = jnp.mean(centered * centered, axis=-1, keepdims=True)
        normed_two = centered * lax.rsqrt(variance + norm_eps) * gain2_ref[...]
        normed_two = normed_two.astype(jnp.bfloat16)
        hidden = matmul(normed_two, fc1_ref[...])
        hidden = 0.5 * hidden * (1.0 + lax.erf(hidden * np.float32(0.5**0.5)))
        blended = first + lax.dot_general(
            hidden.astype(jnp.bfloat16),
            fc2_ref[...],
            (((1,), (1,)), ((), ())),
            preferred_element_type=jnp.float32,
        )
        for place, phase in enumerate(phases):
            at = place * 2 * SIDE
            for slot in range(2):
                rows = blended[at + slot * SIDE : at + (slot + 1) * SIDE]
                target = pl.ds(slots[slot], SIDE, stride=2)
                rows_out[place, 0, target, :] = rows[:, :LANES]
                rows_out[place, 1, target, : features - LANES] = rows[:, LANES:]
            for a in range(WLA):
                for o in range(HALF_LO):
                    row = 2 * octant_row(a, o)
                    pieces = rows_out[place, :, row : row + 2, :].astype(jnp.bfloat16)
                    out_ref[a, phase * HALF_LO + o, :, :LANES] = pieces[0]
                    out_ref[a, phase * HALF_LO + o, :, LANES:] = pieces[1, :, : features - LANES]

    def run_phase(step, _):
        phase = jnp.where(step == 0, near, 1 - near)
        pl.when(step == 0)(lambda: relayed(phase))

        @pl.when(step == 1)
        def _():
            receive(phase, 0)
            for copy in crossings[1]:
                copy.wait_recv()

        receive(phase, 1)
        project(3 * phase)
        attend((phase,))
        return 0

    @pl.when(at_wrap)
    def _():
        lax.fori_loop(0, 2, run_phase, 0)
        pass_on(pl.ds(3 * near, 1), near).wait_send()
        for copy in crossings[1]:
            copy.wait_send()

    @pl.when(jnp.logical_not(at_wrap))
    def _():
        for phase in (1, 0):
            receive(phase, 1)
            relayed(phase)
            project(3 * phase)
        attend((0, 1))
        for phase in range(2):
            pass_on(slice(3 * phase, 3 * phase + 1), phase).wait_send()

    for lon_step in (1, -1):
        for copy in first_parts[lon_step] + last_parts[lon_step]:
            copy.wait_send()
    for copy in row_copies + [own_pass, table_copy]:
        copy.wait_send()


def per_device(
    sizes,
    tokens,
    norm1_gain,
    qkv_weight,
    proj_weight,
    earth_bias,
    norm2_gain,
    fc1_weight,
    fc2_weight,
):
    assert tokens.shape[:3] == (WLV, WLA, WLO)
    assert sizes[0] == 2 and sizes[2] > 3 and earth_bias.shape[0] == 2
    features = tokens.shape[-1]
    assert LANES + LANES // 2 == features
    operands = (
        tokens.transpose(1, 2, 0, 3),
        norm1_gain.reshape(1, -1),
        earth_bias.transpose(1, 2, 0, 3),
        jnp.asarray(toeplitz_matrix(), jnp.bfloat16),
        qkv_weight,
        proj_weight,
        norm2_gain.reshape(1, -1),
        fc1_weight,
        fc2_weight.T,
    )
    assert len(operands) == OPERANDS
    blended = pl.pallas_call(
        functools.partial(kernel, sizes),
        out_shape=jax.ShapeDtypeStruct(operands[0].shape, jnp.bfloat16),
        in_specs=[pl.BlockSpec(memory_space=pltpu.HBM)] * OPERANDS,
        out_specs=pl.BlockSpec(memory_space=pltpu.VMEM),
        scratch_shapes=[
            *[pltpu.VMEM(operand.shape, operand.dtype) for operand in operands],
            pltpu.VMEM((2, 2, SIDE, features), jnp.float32),
            pltpu.VMEM((4, KINDS, 4, PITCH, LANES), jnp.bfloat16),
            pltpu.VMEM((WLV, ROWS, earth_bias.shape[-1]), jnp.float32),
            pltpu.VMEM((3 * ROWS, SECTION), jnp.bfloat16),
            pltpu.VMEM((3 * ROWS, SECTION), jnp.bfloat16),
            pltpu.VMEM((2, 2, 3, STACK, LANES), jnp.float32),
            pltpu.VMEM((2, 2, 2 * LANES, features), jnp.bfloat16),
            pltpu.VMEM((2, 4, STACK, features), jnp.bfloat16),
            pltpu.VMEM((4, 3 * LATS, features), jnp.bfloat16),
            pltpu.VMEM((4, 3 * LATS, features), jnp.bfloat16),
            pltpu.VMEM((2, 2, 2 * SIDE, LANES), jnp.float32),
            pltpu.SemaphoreType.DMA((2, message_count(sizes))),
            pltpu.SemaphoreType.DMA((OPERANDS,)),
            pltpu.SemaphoreType.REGULAR,
            pltpu.VMEM((features, 2 * LANES), jnp.bfloat16),
        ],
        compiler_params=pltpu.CompilerParams(
            collective_id=0, has_side_effects=True, vmem_limit_bytes=48 * 1024 * 1024
        ),
    )(*[pltpu.with_memory_space_constraint(x, pltpu.HBM) for x in operands])
    return blended.transpose(2, 0, 1, 3)


def solution(mesh):
    placed = (
        P("lev", "lat", "lon", None),
        P(),
        P(),
        P(),
        P(None, "lat", None, None),
        P(),
        P(),
        P(),
    )
    return jax.shard_map(
        functools.partial(per_device, tuple(mesh.shape[axis] for axis in AXES)),
        mesh=mesh,
        in_specs=placed,
        out_specs=P("lev", "lat", "lon", None),
        check_vma=False,
    )
```

```python
import functools

import jax
import jax.numpy as jnp
import numpy as np
from jax import lax
from jax.experimental import pallas as pl
from jax.experimental.pallas import tpu as pltpu
from jax.sharding import PartitionSpec as P

HEADS = 6
WLV = 2
WLA = 6
WLO = 12
HALF_LA = WLA // 2
HALF_LO = WLO // 2
OCT = HALF_LA * HALF_LO
PITCH = 24
SIDE = 2 * PITCH
LATS = 2 * SIDE
SPAN = 2 * WLO - 1
CHUNK = WLA * SPAN
ROWS = 8
LANES = 128
AXES = ("lev", "lat", "lon")
OPERANDS = 9
STACK = HEADS * PITCH
SECTION = HALF_LA * CHUNK
KINDS = 5

norm_eps = 1e-05


def octant_row(lat, lon):
    return lat // HALF_LA * PITCH + lat % HALF_LA * HALF_LO + lon % HALF_LO


def toeplitz_matrix():
    pick = np.zeros((CHUNK, WLO * LANES), np.float32)
    for lon in range(WLO):
        for key_lat in range(WLA):
            for key_lon in range(WLO):
                column = lon * LANES + key_lon // HALF_LO * SIDE + octant_row(key_lat, key_lon)
                pick[key_lat * SPAN + lon - key_lon + WLO - 1, column] = 1
    return pick


def matmul(a, b):
    return jnp.dot(a, b, preferred_element_type=jnp.float32)


def lat_moves(size, at):
    stay = (0, 1, 1, 2)
    if size == 2:
        return (stay, (1, 2 - at, 3 * at, 1))
    return (stay, (1, 2, 0, 1), (-1, 1, 3, 1))


def lon_moves():
    return (
        (1, slice(2, 3), slice(0, 1)),
        (-1, slice(1, 2), slice(3, 4)),
        (0, slice(1, 3), slice(1, 3)),
    )


def message_count(sizes):
    lats = len(lat_moves(sizes[1], 0))
    return 4 * lats + (lats - 1) + 3 + 1 + lats


def kernel(sizes, *refs):
    operands, out_ref, held = refs[:OPERANDS], refs[OPERANDS], refs[OPERANDS + 1 : -15]
    (
        own,
        cells,
        tables,
        chunks_out,
        chunks_in,
        bias,
        weights,
        stacked,
        keys,
        values,
        rows_out,
        sems,
        load_sems,
        ready,
        means,
    ) = refs[-15:]
    token_loads = [
        pltpu.make_async_copy(
            operands[0].at[pl.ds(side * HALF_LA, HALF_LA)],
            held[0].at[pl.ds(side * HALF_LA, HALF_LA)],
            load_sems.at[side * OPERANDS],
        )
        for side in range(2)
    ]
    loads = token_loads[:1] + [
        pltpu.make_async_copy(operands[i], held[i], load_sems.at[i]) for i in range(1, OPERANDS)
    ]
    for load in token_loads + loads[1:]:
        load.start()
    (
        tokens_ref,
        gain1_ref,
        table_ref,
        pick_ref,
        qkv_ref,
        proj_ref,
        gain2_ref,
        fc1_ref,
        fc2_ref,
    ) = held
    lev, lat, lon = where = [lax.axis_index(axis) for axis in AXES]
    features = own.shape[-1]
    slots = (lev, 1 - lev)

    def device(steps):
        return {
            axis: lax.rem(at + step + size, size)
            for axis, at, step, size in zip(AXES, where, steps, sizes)
        }

    moves = lat_moves(sizes[1], lat)
    per_side = 2 * len(moves)

    def remote(source, target, index, there):
        return pltpu.make_async_remote_copy(
            src_ref=source,
            dst_ref=target,
            send_sem=sems.at[0, index],
            recv_sem=sems.at[1, index],
            device_id=there,
            device_id_type=pl.DeviceIdType.MESH,
        )

    def part_of(columns, kinds, octants):
        return cells.at[columns, kinds, octants, 0:OCT, :]

    tail_kinds, plain_kind, passed_kinds = slice(1, 3), slice(0, 1), slice(3, 5)
    first_parts, last_parts, peers = {}, {}, {}
    for side, (lon_step, lon_from, lon_to) in enumerate(lon_moves()[:2]):
        first_parts[lon_step], last_parts[lon_step], peers[lon_step] = [], [], []
        for at, (lat_step, lat_from, lat_to, octants) in enumerate(moves):
            there = device((0, lat_step, lon_step))
            peers[lon_step].append(there)
            for part, kinds in enumerate((tail_kinds, plain_kind)):
                (first_parts, last_parts)[part][lon_step].append(
                    remote(
                        part_of(lon_from, kinds, pl.ds(lat_from, octants)),
                        part_of(lon_to, kinds, pl.ds(lat_to, octants)),
                        side * per_side + at * 2 + part,
                        there,
                    )
                )
    row_copies, row_peers = [], []
    for at, (lat_step, lat_from, lat_to, octants) in enumerate(moves[1:]):
        row_peers.append(device((0, lat_step, 0)))
        row_copies.append(
            remote(
                part_of(slice(1, 3), slice(0, 3), pl.ds(lat_from, octants)),
                part_of(slice(1, 3), slice(0, 3), pl.ds(lat_to, octants)),
                2 * per_side + at,
                row_peers[-1],
            )
        )
    partner = device((1, 0, 0))
    passed = 2 * per_side + len(row_copies)
    used = pl.ds(1 - lat, 3) if sizes[1] == 2 else slice(0, 4)

    def pass_on(columns, index):
        return remote(
            part_of(columns, tail_kinds, used),
            part_of(columns, passed_kinds, used),
            passed + index,
            partner,
        )

    own_pass = pass_on(slice(1, 3), 2)
    table_copy = remote(chunks_out, chunks_in, passed + 3, device((0, 1, 0)))
    crossings, cross_peers = {}, {}
    for lon_step, lon_from, lon_to in lon_moves()[:2]:
        crossings[lon_step], cross_peers[lon_step] = [], []
        for at, (lat_step, lat_from, lat_to, octants) in enumerate(moves):
            there = device((1, lat_step, lon_step))
            cross_peers[lon_step].append(there)
            crossings[lon_step].append(
                remote(
                    part_of(lon_from, tail_kinds, pl.ds(lat_from, octants)),
                    part_of(lon_to, passed_kinds, pl.ds(lat_to, octants)),
                    passed + 4 + at,
                    there,
                )
            )

    barrier = pltpu.get_barrier_semaphore()
    first_lon, last_lon = lon == 0, lon == sizes[2] - 1
    before_last = lon == sizes[2] - 2
    at_wrap = first_lon | last_lon

    def tell(semaphore, group):
        for there in group:
            pl.semaphore_signal(
                semaphore, inc=1, device_id=there, device_id_type=pl.DeviceIdType.MESH
            )

    def start(*groups):
        for group in groups:
            for copy in group:
                copy.start()

    wrapped = len(moves)
    greetings = len(row_peers) + 1 + 2 * wrapped
    tell(barrier, peers[-1])
    pl.when(first_lon)(lambda: tell(barrier, cross_peers[-1]))
    pl.when(last_lon)(lambda: tell(barrier, [device((1, 0, -1))]))
    pl.when(jnp.logical_not(last_lon))(lambda: tell(barrier, row_peers + [partner]))
    pl.when(jnp.logical_not(last_lon | before_last))(lambda: tell(barrier, peers[1]))

    cells[:, :, :, OCT:, :] = jnp.zeros((4, KINDS, 4, PITCH - OCT, LANES), jnp.bfloat16)
    for pad in (OCT, PITCH + OCT):
        own[:, :, pad : pad + PITCH - OCT, :] = jnp.zeros(
            (2, 2, PITCH - OCT, features), jnp.float32
        )
    if sizes[1] == 2:
        blank = jnp.zeros((4, KINDS, PITCH, LANES), jnp.bfloat16)

        def clear_low():
            cells[:, :, 0] = blank

        def clear_high():
            cells[:, :, 3] = blank

        pl.when(lat == 0)(clear_low)
        pl.when(lat == 1)(clear_high)

    @pl.when(last_lon)
    def _():
        pl.semaphore_wait(barrier, 2 * wrapped)
        tell(ready, peers[1] + cross_peers[1])

    for a in range(WLA):
        if a % HALF_LA == 0:
            token_loads[a // HALF_LA].wait()
        for o in range(WLO):
            cell = tokens_ref[a, o].astype(jnp.float32)
            row = octant_row(a, o)
            for side in range(WLV):
                own[o // HALF_LO, slots[side], row : row + 1, :] = cell[side : side + 1]
    loads[1].wait()
    raw = own[...].reshape(4 * SIDE, features)
    averages = jnp.mean(raw, axis=-1, keepdims=True)
    normed = raw - averages
    scales = lax.rsqrt(jnp.mean(normed * normed, axis=-1, keepdims=True) + norm_eps)
    normed = normed * scales * gain1_ref[...]
    lower = lax.broadcasted_iota(jnp.int32, (SIDE, LANES), 1) < features - LANES
    tail_gain = jnp.concatenate([gain1_ref[:, LANES:]] * 2, axis=1)
    for half in range(2):
        pair = [slice(at, at + SIDE) for at in (half * 2 * SIDE, (half * 2 + 1) * SIDE)]
        tails = jnp.concatenate([raw[rows, LANES:] for rows in pair], axis=1)
        average, by = (
            jnp.where(lower, found[pair[0]], found[pair[1]]) for found in (averages, scales)
        )
        tails = (tails - average) * by * tail_gain
        for kind, block in enumerate((normed[pair[0], :LANES], normed[pair[1], :LANES], tails)):
            cells[1 + half, kind, 1:3] = block.reshape(2, PITCH, LANES).astype(jnp.bfloat16)
    normed = normed.astype(jnp.bfloat16)

    def over_wrap(lon_step, at_lat, at_lev):
        own = [first_parts[lon_step], last_parts[lon_step]]
        for to_lat in range(2):
            index = at_lat ^ to_lat
            groups = [own, [crossings[lon_step]]]
            for group in groups[at_lev], groups[1 - at_lev]:
                for copies in group:
                    copies[index].start()

    def send_over_wrap(lon_step, order):
        if sizes[1] != 2:
            start(first_parts[lon_step], last_parts[lon_step], crossings[lon_step])
            return
        for at_lat in range(2):
            for at_lev in range(2):
                pl.when((lat == at_lat) & (lev == at_lev))(
                    functools.partial(over_wrap, lon_step, at_lat, at_lev ^ order)
                )

    pl.when(last_lon)(lambda: send_over_wrap(1, 0))

    @pl.when(jnp.logical_not(last_lon))
    def _():
        expected = jnp.where(first_lon, greetings - wrapped, greetings)
        pl.semaphore_wait(barrier, jnp.where(before_last, greetings + 1, expected))
        pl.when(before_last)(lambda: tell(ready, peers[1]))
        pl.when(jnp.logical_not(first_lon))(lambda: start(first_parts[-1], last_parts[-1]))
        start(row_copies, first_parts[1], last_parts[1])

    loads[2].wait()
    tables[...] = jnp.zeros_like(tables)
    for head in range(HEADS):
        pair = table_ref[0, head].astype(jnp.float32)
        for kind in range(WLV):
            tables[kind, head : head + 1, :] = pair[kind : kind + 1]

    def section(kind, query_lev, key_lev, side):
        at = (query_lev * WLV + key_lev) * WLA * CHUNK + side * SECTION
        return tables[kind, :, at : at + SECTION]

    def sections(side):
        found = [
            jnp.where(lev == 0, section(kind, *low, side), section(kind, *high, side))
            for kind, low, high in ((1, (1, 1), (0, 0)), (0, (0, 0), (1, 1)), (0, (0, 1), (1, 0)))
        ]
        return jnp.concatenate(found, axis=0)

    chunks_out[...] = sections(1).astype(jnp.bfloat16)
    pl.when(jnp.logical_not(last_lon))(table_copy.start)
    own_chunks = sections(0)

    lane = lax.broadcasted_iota(jnp.int32, (ROWS, LANES), 1)
    lat_side = lane % SIDE // PITCH
    real = (lane < LATS) & (lane % PITCH < OCT)
    partner_out = (lat == 0, lat == sizes[1] - 1)

    def fill_bias(half, found):
        chunk_rows = jnp.concatenate(
            [found[:, step * CHUNK : (step + 1) * CHUNK] for step in range(HALF_LA)], axis=0
        )
        spread = matmul(chunk_rows.astype(jnp.bfloat16), pick_ref[...])
        allowed = real & ((lat_side != half) | jnp.logical_not(partner_out[half]))
        for step in range(HALF_LA):
            for kind in range(3):
                at = (step * 3 + kind) * ROWS
                for o in range(WLO):
                    tile = spread[at : at + ROWS, o * LANES : (o + 1) * LANES]
                    tile = jnp.where(allowed, tile, -1e30)
                    bias[
                        1 - o // HALF_LO,
                        half,
                        kind,
                        pl.ds(step * HALF_LO + o % HALF_LO, HEADS, stride=PITCH),
                        :,
                    ] = tile[:HEADS]

    loads[3].wait()
    fill_bias(1, own_chunks)

    loads[4].wait()
    for part in range(2):
        weight = qkv_ref[:, (part + 1) * features : (part + 2) * features]
        blank_rows = jnp.zeros((features - LANES, features), jnp.bfloat16)
        for slot in range(2):
            weights[part, slot, :LANES] = weight[:LANES]
            pieces = (weight[LANES:], blank_rows)
            for place in range(2):
                at = LANES + place * (features - LANES)
                weights[part, slot, at : at + features - LANES] = pieces[place ^ slot]
    queries = matmul(normed, qkv_ref[:, :features])
    head_of = lax.broadcasted_iota(jnp.int32, (PITCH, features), 1) // (features // HEADS)
    for octant in range(8):
        rows = queries[octant * PITCH : (octant + 1) * PITCH]
        stacked[octant // 4, octant % 4] = jnp.concatenate(
            [jnp.where(head_of == head, rows, 0.0) for head in range(HEADS)], axis=0
        ).astype(jnp.bfloat16)

    def project(column):
        plain, paired, tails, passed_on, passed_tails = (
            cells[column, kind].reshape(LATS, LANES) for kind in range(KINDS)
        )
        plain = jnp.concatenate([plain, tails], axis=1)
        paired = jnp.concatenate(
            [
                jnp.concatenate([paired, tails], axis=1),
                jnp.concatenate([passed_on, passed_tails], axis=1),
            ],
            axis=0,
        )
        for part, kept in enumerate((keys, values)):
            kept[column, :LATS] = matmul(plain, weights[part, 0]).astype(jnp.bfloat16)
            kept[column, LATS:] = matmul(paired, weights[part, 1]).astype(jnp.bfloat16)

    def receive(phase, part):
        for at, (_, lat_from, lat_to, octants) in enumerate(moves):
            kinds = (tail_kinds, plain_kind)[part]
            remote(
                part_of(slice(1, 2), kinds, pl.ds(lat_from, octants)),
                part_of(pl.ds(3 * phase, 1), kinds, pl.ds(lat_to, octants)),
                phase * per_side + at * 2 + part,
                partner,
            ).wait_recv()

    def relay(phase):
        receive(phase, 0)
        pass_on(pl.ds(3 * phase, 1), phase).start()

    def relayed(phase):
        pass_on(pl.ds(3 * phase, 1), phase).wait_recv()

    near = jnp.where(last_lon, 0, 1)

    @pl.when(last_lon)
    def _():
        pl.semaphore_wait(ready, wrapped)
        start(row_copies, [table_copy], first_parts[-1], last_parts[-1])

    for copy in row_copies:
        copy.wait_recv()
    own_pass.start()
    @pl.when(first_lon)
    def _():
        pl.semaphore_wait(ready, 2 * wrapped)
        send_over_wrap(-1, 1)

    relay(near)
    pl.when(jnp.logical_not(at_wrap))(lambda: relay(1 - near))
    table_copy.wait_recv()
    fill_bias(0, chunks_in[...].astype(jnp.float32))
    own_pass.wait_recv()
    for column in (1, 2):
        project(column)
    for load in loads[5:]:
        load.wait()
    row_mean = jnp.mean(proj_ref[...].astype(jnp.float32), axis=-1, keepdims=True)
    high_part = row_mean.astype(jnp.bfloat16)
    low_part = (row_mean - high_part.astype(jnp.float32)).astype(jnp.bfloat16)
    for part, column in enumerate((high_part, low_part)):
        means[:, part * LANES : (part + 1) * LANES] = jnp.broadcast_to(column, (features, LANES))

    scale = (features // HEADS) ** (-0.5)
    rest = jnp.zeros((LANES - LATS, features), jnp.bfloat16)

    def window_rows(held_rows, phase, slot, half):
        at = slot * LATS + half * SIDE
        pieces = [held_rows[2 * phase + side, at : at + SIDE, :] for side in range(2)]
        return pieces + [rest]

    def attend(phases):
        octants = [(p, slot, half) for p in phases for slot in range(2) for half in range(2)]
        slot_keys = ((0,), (1, 2))

        def window(held_rows, phase, slot, half):
            return jnp.concatenate(
                [r for s in slot_keys[slot] for r in window_rows(held_rows, phase, s, half)], axis=0
            )

        scores = [
            lax.dot_general(
                stacked[phase, slot * 2 + half],
                window(keys, phase, slot, half),
                (((1,), (1,)), ((), ())),
                preferred_element_type=jnp.float32,
            )
            for phase, slot, half in octants
        ]
        shares, totals = [], []
        for (phase, slot, half), products in zip(octants, scores):
            added = jnp.concatenate([bias[phase, half, s] for s in slot_keys[slot]], axis=1)
            products = products * scale + added
            weight = jnp.exp(products - jnp.max(products, axis=-1, keepdims=True))
            shares.append(weight.astype(jnp.bfloat16))
            totals.append(jnp.sum(weight, axis=-1, keepdims=True))
        mixes = [
            matmul(weight, window(values, phase, slot, half))
            for (phase, slot, half), weight in zip(octants, shares)
        ]
        found = []
        for mixed, total in zip(mixes, totals):
            mixed = mixed * (1.0 / total)
            found.append(
                sum(
                    jnp.where(head_of == head, mixed[head * PITCH : (head + 1) * PITCH], 0.0)
                    for head in range(HEADS)
                )
            )
        context = jnp.concatenate(found, axis=0).astype(jnp.bfloat16)
        tokens = jnp.concatenate([own[p].reshape(4 * PITCH, features) for p in phases], axis=0)
        average = matmul(context, means[...])
        average = average[:, :LANES] + average[:, LANES:]
        average = average + jnp.mean(tokens, axis=-1, keepdims=True)
        first = tokens + matmul(context, proj_ref[...])
        centered = first - jnp.concatenate([average, average[:, : features - LANES]], axis=1)
        variance = jnp.mean(centered * centered, axis=-1, keepdims=True)
        normed_two = centered * lax.rsqrt(variance + norm_eps) * gain2_ref[...]
        normed_two = normed_two.astype(jnp.bfloat16)
        hidden = matmul(normed_two, fc1_ref[...])
        hidden = 0.5 * hidden * (1.0 + lax.erf(hidden * np.float32(0.5**0.5)))
        blended = first + lax.dot_general(
            hidden.astype(jnp.bfloat16),
            fc2_ref[...],
            (((1,), (1,)), ((), ())),
            preferred_element_type=jnp.float32,
        )
        for place, phase in enumerate(phases):
            at = place * 2 * SIDE
            for slot in range(2):
                rows = blended[at + slot * SIDE : at + (slot + 1) * SIDE]
                target = pl.ds(slots[slot], SIDE, stride=2)
                rows_out[place, 0, target, :] = rows[:, :LANES]
                rows_out[place, 1, target, : features - LANES] = rows[:, LANES:]
            for a in range(WLA):
                for o in range(HALF_LO):
                    row = 2 * octant_row(a, o)
                    pieces = rows_out[place, :, row : row + 2, :].astype(jnp.bfloat16)
                    out_ref[a, phase * HALF_LO + o, :, :LANES] = pieces[0]
                    out_ref[a, phase * HALF_LO + o, :, LANES:] = pieces[1, :, : features - LANES]

    def run_phase(step, _):
        phase = jnp.where(step == 0, near, 1 - near)
        pl.when(step == 0)(lambda: relayed(phase))

        @pl.when(step == 1)
        def _():
            receive(phase, 0)
            for copy in crossings[1]:
                copy.wait_recv()

        receive(phase, 1)
        project(3 * phase)
        attend((phase,))
        return 0

    @pl.when(at_wrap)
    def _():
        lax.fori_loop(0, 2, run_phase, 0)
        pass_on(pl.ds(3 * near, 1), near).wait_send()
        for copy in crossings[1]:
            copy.wait_send()

    @pl.when(jnp.logical_not(at_wrap))
    def _():
        for phase in (1, 0):
            receive(phase, 1)
            relayed(phase)
            project(3 * phase)
        attend((0, 1))
        for phase in range(2):
            pass_on(slice(3 * phase, 3 * phase + 1), phase).wait_send()

    for lon_step in (1, -1):
        for copy in first_parts[lon_step] + last_parts[lon_step]:
            copy.wait_send()
    for copy in row_copies + [own_pass, table_copy]:
        copy.wait_send()


def per_device(
    sizes,
    tokens,
    norm1_gain,
    qkv_weight,
    proj_weight,
    earth_bias,
    norm2_gain,
    fc1_weight,
    fc2_weight,
):
    assert tokens.shape[:3] == (WLV, WLA, WLO)
    assert sizes[0] == 2 and sizes[2] > 3 and earth_bias.shape[0] == 2
    features = tokens.shape[-1]
    assert LANES + LANES // 2 == features
    operands = (
        tokens.transpose(1, 2, 0, 3),
        norm1_gain.reshape(1, -1),
        earth_bias.transpose(1, 2, 0, 3),
        jnp.asarray(toeplitz_matrix(), jnp.bfloat16),
        qkv_weight,
        proj_weight,
        norm2_gain.reshape(1, -1),
        fc1_weight,
        fc2_weight.T,
    )
    assert len(operands) == OPERANDS
    blended = pl.pallas_call(
        functools.partial(kernel, sizes),
        out_shape=jax.ShapeDtypeStruct(operands[0].shape, jnp.bfloat16),
        in_specs=[pl.BlockSpec(memory_space=pltpu.HBM)] * OPERANDS,
        out_specs=pl.BlockSpec(memory_space=pltpu.VMEM),
        scratch_shapes=[
            *[pltpu.VMEM(operand.shape, operand.dtype) for operand in operands],
            pltpu.VMEM((2, 2, SIDE, features), jnp.float32),
            pltpu.VMEM((4, KINDS, 4, PITCH, LANES), jnp.bfloat16),
            pltpu.VMEM((WLV, ROWS, earth_bias.shape[-1]), jnp.float32),
            pltpu.VMEM((3 * ROWS, SECTION), jnp.bfloat16),
            pltpu.VMEM((3 * ROWS, SECTION), jnp.bfloat16),
            pltpu.VMEM((2, 2, 3, STACK, LANES), jnp.float32),
            pltpu.VMEM((2, 2, 2 * LANES, features), jnp.bfloat16),
            pltpu.VMEM((2, 4, STACK, features), jnp.bfloat16),
            pltpu.VMEM((4, 3 * LATS, features), jnp.bfloat16),
            pltpu.VMEM((4, 3 * LATS, features), jnp.bfloat16),
            pltpu.VMEM((2, 2, 2 * SIDE, LANES), jnp.float32),
            pltpu.SemaphoreType.DMA((2, message_count(sizes))),
            pltpu.SemaphoreType.DMA((OPERANDS + 1,)),
            pltpu.SemaphoreType.REGULAR,
            pltpu.VMEM((features, 2 * LANES), jnp.bfloat16),
        ],
        compiler_params=pltpu.CompilerParams(
            collective_id=0, has_side_effects=True, vmem_limit_bytes=48 * 1024 * 1024
        ),
    )(*[pltpu.with_memory_space_constraint(x, pltpu.HBM) for x in operands])
    return blended.transpose(2, 0, 1, 3)


def solution(mesh):
    placed = (
        P("lev", "lat", "lon", None),
        P(),
        P(),
        P(),
        P(None, "lat", None, None),
        P(),
        P(),
        P(),
    )
    return jax.shard_map(
        functools.partial(per_device, tuple(mesh.shape[axis] for axis in AXES)),
        mesh=mesh,
        in_specs=placed,
        out_specs=P("lev", "lat", "lon", None),
        check_vma=False,
    )
```

```python
import functools

import jax
import jax.numpy as jnp
import numpy as np
from jax import lax
from jax.experimental import pallas as pl
from jax.experimental.pallas import tpu as pltpu
from jax.sharding import PartitionSpec as P

HEADS = 6
WLV = 2
WLA = 6
WLO = 12
HALF_LA = WLA // 2
HALF_LO = WLO // 2
OCT = HALF_LA * HALF_LO
PITCH = 24
SIDE = 2 * PITCH
LATS = 2 * SIDE
SPAN = 2 * WLO - 1
CHUNK = WLA * SPAN
ROWS = 8
LANES = 128
AXES = ("lev", "lat", "lon")
OPERANDS = 9
STACK = HEADS * PITCH
SECTION = HALF_LA * CHUNK
KINDS = 5
LOAD_ROWS = 2

norm_eps = 1e-05


def octant_row(lat, lon):
    return lat // HALF_LA * PITCH + lat % HALF_LA * HALF_LO + lon % HALF_LO


def toeplitz_matrix():
    pick = np.zeros((CHUNK, WLO * LANES), np.float32)
    for lon in range(WLO):
        for key_lat in range(WLA):
            for key_lon in range(WLO):
                column = lon * LANES + key_lon // HALF_LO * SIDE + octant_row(key_lat, key_lon)
                pick[key_lat * SPAN + lon - key_lon + WLO - 1, column] = 1
    return pick


def matmul(a, b):
    return jnp.dot(a, b, preferred_element_type=jnp.float32)


def lat_moves(size, at):
    stay = (0, 1, 1, 2)
    if size == 2:
        return (stay, (1, 2 - at, 3 * at, 1))
    return (stay, (1, 2, 0, 1), (-1, 1, 3, 1))


def lon_moves():
    return (
        (1, slice(2, 3), slice(0, 1)),
        (-1, slice(1, 2), slice(3, 4)),
        (0, slice(1, 3), slice(1, 3)),
    )


def message_count(sizes):
    lats = len(lat_moves(sizes[1], 0))
    return 4 * lats + (lats - 1) + 3 + 1 + lats


def kernel(sizes, *refs):
    operands, out_ref, held = refs[:OPERANDS], refs[OPERANDS], refs[OPERANDS + 1 : -15]
    (
        own,
        cells,
        tables,
        chunks_out,
        chunks_in,
        bias,
        weights,
        stacked,
        keys,
        values,
        rows_out,
        sems,
        load_sems,
        ready,
        means,
    ) = refs[-15:]
    token_loads = [
        pltpu.make_async_copy(
            operands[0].at[pl.ds(part * LOAD_ROWS, LOAD_ROWS)],
            held[0].at[pl.ds(part * LOAD_ROWS, LOAD_ROWS)],
            load_sems.at[OPERANDS - 1 + part if part else 0],
        )
        for part in range(WLA // LOAD_ROWS)
    ]
    loads = token_loads[:1] + [
        pltpu.make_async_copy(operands[i], held[i], load_sems.at[i]) for i in range(1, OPERANDS)
    ]
    for load in token_loads + loads[1:]:
        load.start()
    (
        tokens_ref,
        gain1_ref,
        table_ref,
        pick_ref,
        qkv_ref,
        proj_ref,
        gain2_ref,
        fc1_ref,
        fc2_ref,
    ) = held
    lev, lat, lon = where = [lax.axis_index(axis) for axis in AXES]
    features = own.shape[-1]
    slots = (lev, 1 - lev)

    def device(steps):
        return {
            axis: lax.rem(at + step + size, size)
            for axis, at, step, size in zip(AXES, where, steps, sizes)
        }

    moves = lat_moves(sizes[1], lat)
    per_side = 2 * len(moves)

    def remote(source, target, index, there):
        return pltpu.make_async_remote_copy(
            src_ref=source,
            dst_ref=target,
            send_sem=sems.at[0, index],
            recv_sem=sems.at[1, index],
            device_id=there,
            device_id_type=pl.DeviceIdType.MESH,
        )

    def part_of(columns, kinds, octants):
        return cells.at[columns, kinds, octants, 0:OCT, :]

    tail_kinds, plain_kind, passed_kinds = slice(1, 3), slice(0, 1), slice(3, 5)
    first_parts, last_parts, peers = {}, {}, {}
    for side, (lon_step, lon_from, lon_to) in enumerate(lon_moves()[:2]):
        first_parts[lon_step], last_parts[lon_step], peers[lon_step] = [], [], []
        for at, (lat_step, lat_from, lat_to, octants) in enumerate(moves):
            there = device((0, lat_step, lon_step))
            peers[lon_step].append(there)
            for part, kinds in enumerate((tail_kinds, plain_kind)):
                (first_parts, last_parts)[part][lon_step].append(
                    remote(
                        part_of(lon_from, kinds, pl.ds(lat_from, octants)),
                        part_of(lon_to, kinds, pl.ds(lat_to, octants)),
                        side * per_side + at * 2 + part,
                        there,
                    )
                )
    row_copies, row_peers = [], []
    for at, (lat_step, lat_from, lat_to, octants) in enumerate(moves[1:]):
        row_peers.append(device((0, lat_step, 0)))
        row_copies.append(
            remote(
                part_of(slice(1, 3), slice(0, 3), pl.ds(lat_from, octants)),
                part_of(slice(1, 3), slice(0, 3), pl.ds(lat_to, octants)),
                2 * per_side + at,
                row_peers[-1],
            )
        )
    partner = device((1, 0, 0))
    passed = 2 * per_side + len(row_copies)
    used = pl.ds(1 - lat, 3) if sizes[1] == 2 else slice(0, 4)

    def pass_on(columns, index):
        return remote(
            part_of(columns, tail_kinds, used),
            part_of(columns, passed_kinds, used),
            passed + index,
            partner,
        )

    own_pass = pass_on(slice(1, 3), 2)
    table_copy = remote(chunks_out, chunks_in, passed + 3, device((0, 1, 0)))
    crossings, cross_peers = {}, {}
    for lon_step, lon_from, lon_to in lon_moves()[:2]:
        crossings[lon_step], cross_peers[lon_step] = [], []
        for at, (lat_step, lat_from, lat_to, octants) in enumerate(moves):
            there = device((1, lat_step, lon_step))
            cross_peers[lon_step].append(there)
            crossings[lon_step].append(
                remote(
                    part_of(lon_from, tail_kinds, pl.ds(lat_from, octants)),
                    part_of(lon_to, passed_kinds, pl.ds(lat_to, octants)),
                    passed + 4 + at,
                    there,
                )
            )

    barrier = pltpu.get_barrier_semaphore()
    first_lon, last_lon = lon == 0, lon == sizes[2] - 1
    before_last = lon == sizes[2] - 2
    at_wrap = first_lon | last_lon

    def tell(semaphore, group):
        for there in group:
            pl.semaphore_signal(
                semaphore, inc=1, device_id=there, device_id_type=pl.DeviceIdType.MESH
            )

    def start(*groups):
        for group in groups:
            for copy in group:
                copy.start()

    wrapped = len(moves)
    greetings = len(row_peers) + 1 + 2 * wrapped
    tell(barrier, peers[-1])
    pl.when(first_lon)(lambda: tell(barrier, cross_peers[-1]))
    pl.when(last_lon)(lambda: tell(barrier, [device((1, 0, -1))]))
    pl.when(jnp.logical_not(last_lon))(lambda: tell(barrier, row_peers + [partner]))
    pl.when(jnp.logical_not(last_lon | before_last))(lambda: tell(barrier, peers[1]))

    cells[:, :, :, OCT:, :] = jnp.zeros((4, KINDS, 4, PITCH - OCT, LANES), jnp.bfloat16)
    for pad in (OCT, PITCH + OCT):
        own[:, :, pad : pad + PITCH - OCT, :] = jnp.zeros(
            (2, 2, PITCH - OCT, features), jnp.float32
        )
    if sizes[1] == 2:
        blank = jnp.zeros((4, KINDS, PITCH, LANES), jnp.bfloat16)

        def clear_low():
            cells[:, :, 0] = blank

        def clear_high():
            cells[:, :, 3] = blank

        pl.when(lat == 0)(clear_low)
        pl.when(lat == 1)(clear_high)

    @pl.when(last_lon)
    def _():
        pl.semaphore_wait(barrier, 2 * wrapped)
        tell(ready, peers[1] + cross_peers[1])

    for a in range(WLA):
        if a % LOAD_ROWS == 0:
            token_loads[a // LOAD_ROWS].wait()
        for o in range(WLO):
            cell = tokens_ref[a, o].astype(jnp.float32)
            row = octant_row(a, o)
            for side in range(WLV):
                own[o // HALF_LO, slots[side], row : row + 1, :] = cell[side : side + 1]
    loads[1].wait()
    raw = own[...].reshape(4 * SIDE, features)
    averages = jnp.mean(raw, axis=-1, keepdims=True)
    normed = raw - averages
    scales = lax.rsqrt(jnp.mean(normed * normed, axis=-1, keepdims=True) + norm_eps)
    normed = normed * scales * gain1_ref[...]
    lower = lax.broadcasted_iota(jnp.int32, (SIDE, LANES), 1) < features - LANES
    tail_gain = jnp.concatenate([gain1_ref[:, LANES:]] * 2, axis=1)
    for half in range(2):
        pair = [slice(at, at + SIDE) for at in (half * 2 * SIDE, (half * 2 + 1) * SIDE)]
        tails = jnp.concatenate([raw[rows, LANES:] for rows in pair], axis=1)
        average, by = (
            jnp.where(lower, found[pair[0]], found[pair[1]]) for found in (averages, scales)
        )
        tails = (tails - average) * by * tail_gain
        for kind, block in enumerate((normed[pair[0], :LANES], normed[pair[1], :LANES], tails)):
            cells[1 + half, kind, 1:3] = block.reshape(2, PITCH, LANES).astype(jnp.bfloat16)
    normed = normed.astype(jnp.bfloat16)

    def over_wrap(lon_step, at_lat, at_lev):
        own = [first_parts[lon_step], last_parts[lon_step]]
        for to_lat in range(2):
            index = at_lat ^ to_lat
            groups = [own, [crossings[lon_step]]]
            for group in groups[at_lev], groups[1 - at_lev]:
                for copies in group:
                    copies[index].start()

    def send_over_wrap(lon_step, order):
        if sizes[1] != 2:
            start(first_parts[lon_step], last_parts[lon_step], crossings[lon_step])
            return
        for at_lat in range(2):
            for at_lev in range(2):
                pl.when((lat == at_lat) & (lev == at_lev))(
                    functools.partial(over_wrap, lon_step, at_lat, at_lev ^ order)
                )

    pl.when(last_lon)(lambda: send_over_wrap(1, 0))

    @pl.when(jnp.logical_not(last_lon))
    def _():
        expected = jnp.where(first_lon, greetings - wrapped, greetings)
        pl.semaphore_wait(barrier, jnp.where(before_last, greetings + 1, expected))
        pl.when(before_last)(lambda: tell(ready, peers[1]))
        pl.when(jnp.logical_not(first_lon))(lambda: start(first_parts[-1], last_parts[-1]))
        start(row_copies, first_parts[1], last_parts[1])

    loads[2].wait()
    tables[...] = jnp.zeros_like(tables)
    for head in range(HEADS):
        pair = table_ref[0, head].astype(jnp.float32)
        for kind in range(WLV):
            tables[kind, head : head + 1, :] = pair[kind : kind + 1]

    def section(kind, query_lev, key_lev, side):
        at = (query_lev * WLV + key_lev) * WLA * CHUNK + side * SECTION
        return tables[kind, :, at : at + SECTION]

    def sections(side):
        found = [
            jnp.where(lev == 0, section(kind, *low, side), section(kind, *high, side))
            for kind, low, high in ((1, (1, 1), (0, 0)), (0, (0, 0), (1, 1)), (0, (0, 1), (1, 0)))
        ]
        return jnp.concatenate(found, axis=0)

    chunks_out[...] = sections(1).astype(jnp.bfloat16)
    pl.when(jnp.logical_not(last_lon))(table_copy.start)
    own_chunks = sections(0)

    lane = lax.broadcasted_iota(jnp.int32, (ROWS, LANES), 1)
    lat_side = lane % SIDE // PITCH
    real = (lane < LATS) & (lane % PITCH < OCT)
    partner_out = (lat == 0, lat == sizes[1] - 1)

    def fill_bias(half, found):
        chunk_rows = jnp.concatenate(
            [found[:, step * CHUNK : (step + 1) * CHUNK] for step in range(HALF_LA)], axis=0
        )
        spread = matmul(chunk_rows.astype(jnp.bfloat16), pick_ref[...])
        allowed = real & ((lat_side != half) | jnp.logical_not(partner_out[half]))
        for step in range(HALF_LA):
            for kind in range(3):
                at = (step * 3 + kind) * ROWS
                for o in range(WLO):
                    tile = spread[at : at + ROWS, o * LANES : (o + 1) * LANES]
                    tile = jnp.where(allowed, tile, -1e30)
                    bias[
                        1 - o // HALF_LO,
                        half,
                        kind,
                        pl.ds(step * HALF_LO + o % HALF_LO, HEADS, stride=PITCH),
                        :,
                    ] = tile[:HEADS]

    loads[3].wait()
    fill_bias(1, own_chunks)

    loads[4].wait()
    for part in range(2):
        weight = qkv_ref[:, (part + 1) * features : (part + 2) * features]
        blank_rows = jnp.zeros((features - LANES, features), jnp.bfloat16)
        for slot in range(2):
            weights[part, slot, :LANES] = weight[:LANES]
            pieces = (weight[LANES:], blank_rows)
            for place in range(2):
                at = LANES + place * (features - LANES)
                weights[part, slot, at : at + features - LANES] = pieces[place ^ slot]
    queries = matmul(normed, qkv_ref[:, :features])
    head_of = lax.broadcasted_iota(jnp.int32, (PITCH, features), 1) // (features // HEADS)
    for octant in range(8):
        rows = queries[octant * PITCH : (octant + 1) * PITCH]
        stacked[octant // 4, octant % 4] = jnp.concatenate(
            [jnp.where(head_of == head, rows, 0.0) for head in range(HEADS)], axis=0
        ).astype(jnp.bfloat16)

    def project(column):
        plain, paired, tails, passed_on, passed_tails = (
            cells[column, kind].reshape(LATS, LANES) for kind in range(KINDS)
        )
        plain = jnp.concatenate([plain, tails], axis=1)
        paired = jnp.concatenate(
            [
                jnp.concatenate([paired, tails], axis=1),
                jnp.concatenate([passed_on, passed_tails], axis=1),
            ],
            axis=0,
        )
        for part, kept in enumerate((keys, values)):
            kept[column, :LATS] = matmul(plain, weights[part, 0]).astype(jnp.bfloat16)
            kept[column, LATS:] = matmul(paired, weights[part, 1]).astype(jnp.bfloat16)

    def receive(phase, part):
        for at, (_, lat_from, lat_to, octants) in enumerate(moves):
            kinds = (tail_kinds, plain_kind)[part]
            remote(
                part_of(slice(1, 2), kinds, pl.ds(lat_from, octants)),
                part_of(pl.ds(3 * phase, 1), kinds, pl.ds(lat_to, octants)),
                phase * per_side + at * 2 + part,
                partner,
            ).wait_recv()

    def relay(phase):
        receive(phase, 0)
        pass_on(pl.ds(3 * phase, 1), phase).start()

    def relayed(phase):
        pass_on(pl.ds(3 * phase, 1), phase).wait_recv()

    near = jnp.where(last_lon, 0, 1)

    @pl.when(last_lon)
    def _():
        pl.semaphore_wait(ready, wrapped)
        start(row_copies, [table_copy], first_parts[-1], last_parts[-1])

    for copy in row_copies:
        copy.wait_recv()
    own_pass.start()
    @pl.when(first_lon)
    def _():
        pl.semaphore_wait(ready, 2 * wrapped)
        send_over_wrap(-1, 1)

    relay(near)
    pl.when(jnp.logical_not(at_wrap))(lambda: relay(1 - near))
    table_copy.wait_recv()
    fill_bias(0, chunks_in[...].astype(jnp.float32))
    own_pass.wait_recv()
    for column in (1, 2):
        project(column)
    for load in loads[5:]:
        load.wait()
    row_mean = jnp.mean(proj_ref[...].astype(jnp.float32), axis=-1, keepdims=True)
    high_part = row_mean.astype(jnp.bfloat16)
    low_part = (row_mean - high_part.astype(jnp.float32)).astype(jnp.bfloat16)
    for part, column in enumerate((high_part, low_part)):
        means[:, part * LANES : (part + 1) * LANES] = jnp.broadcast_to(column, (features, LANES))

    scale = (features // HEADS) ** (-0.5)
    rest = jnp.zeros((LANES - LATS, features), jnp.bfloat16)

    def window_rows(held_rows, phase, slot, half):
        at = slot * LATS + half * SIDE
        pieces = [held_rows[2 * phase + side, at : at + SIDE, :] for side in range(2)]
        return pieces + [rest]

    def attend(phases):
        octants = [(p, slot, half) for p in phases for slot in range(2) for half in range(2)]
        slot_keys = ((0,), (1, 2))

        def window(held_rows, phase, slot, half):
            return jnp.concatenate(
                [r for s in slot_keys[slot] for r in window_rows(held_rows, phase, s, half)], axis=0
            )

        scores = [
            lax.dot_general(
                stacked[phase, slot * 2 + half],
                window(keys, phase, slot, half),
                (((1,), (1,)), ((), ())),
                preferred_element_type=jnp.float32,
            )
            for phase, slot, half in octants
        ]
        shares, totals = [], []
        for (phase, slot, half), products in zip(octants, scores):
            added = jnp.concatenate([bias[phase, half, s] for s in slot_keys[slot]], axis=1)
            products = products * scale + added
            weight = jnp.exp(products - jnp.max(products, axis=-1, keepdims=True))
            shares.append(weight.astype(jnp.bfloat16))
            totals.append(jnp.sum(weight, axis=-1, keepdims=True))
        mixes = [
            matmul(weight, window(values, phase, slot, half))
            for (phase, slot, half), weight in zip(octants, shares)
        ]
        found = []
        for mixed, total in zip(mixes, totals):
            mixed = mixed * (1.0 / total)
            found.append(
                sum(
                    jnp.where(head_of == head, mixed[head * PITCH : (head + 1) * PITCH], 0.0)
                    for head in range(HEADS)
                )
            )
        context = jnp.concatenate(found, axis=0).astype(jnp.bfloat16)
        tokens = jnp.concatenate([own[p].reshape(4 * PITCH, features) for p in phases], axis=0)
        average = matmul(context, means[...])
        average = average[:, :LANES] + average[:, LANES:]
        average = average + jnp.mean(tokens, axis=-1, keepdims=True)
        first = tokens + matmul(context, proj_ref[...])
        centered = first - jnp.concatenate([average, average[:, : features - LANES]], axis=1)
        variance = jnp.mean(centered * centered, axis=-1, keepdims=True)
        normed_two = centered * lax.rsqrt(variance + norm_eps) * gain2_ref[...]
        normed_two = normed_two.astype(jnp.bfloat16)
        hidden = matmul(normed_two, fc1_ref[...])
        hidden = hidden * (1.0 + lax.erf(hidden * np.float32(0.5**0.5)))
        blended = first + 0.5 * lax.dot_general(
            hidden.astype(jnp.bfloat16),
            fc2_ref[...],
            (((1,), (1,)), ((), ())),
            preferred_element_type=jnp.float32,
        )
        for place, phase in enumerate(phases):
            at = place * 2 * SIDE
            for slot in range(2):
                rows = blended[at + slot * SIDE : at + (slot + 1) * SIDE]
                target = pl.ds(slots[slot], SIDE, stride=2)
                rows_out[place, 0, target, :] = rows[:, :LANES]
                rows_out[place, 1, target, : features - LANES] = rows[:, LANES:]
            for a in range(WLA):
                for o in range(HALF_LO):
                    row = 2 * octant_row(a, o)
                    pieces = rows_out[place, :, row : row + 2, :].astype(jnp.bfloat16)
                    out_ref[a, phase * HALF_LO + o, :, :LANES] = pieces[0]
                    out_ref[a, phase * HALF_LO + o, :, LANES:] = pieces[1, :, : features - LANES]

    def run_phase(step, _):
        phase = jnp.where(step == 0, near, 1 - near)
        pl.when(step == 0)(lambda: relayed(phase))

        @pl.when(step == 1)
        def _():
            receive(phase, 0)
            for copy in crossings[1]:
                copy.wait_recv()

        receive(phase, 1)
        project(3 * phase)
        attend((phase,))
        return 0

    @pl.when(at_wrap)
    def _():
        lax.fori_loop(0, 2, run_phase, 0)
        pass_on(pl.ds(3 * near, 1), near).wait_send()
        for copy in crossings[1]:
            copy.wait_send()

    @pl.when(jnp.logical_not(at_wrap))
    def _():
        for phase in (1, 0):
            receive(phase, 1)
            relayed(phase)
            project(3 * phase)
        attend((0, 1))
        for phase in range(2):
            pass_on(slice(3 * phase, 3 * phase + 1), phase).wait_send()

    for lon_step in (1, -1):
        for copy in first_parts[lon_step] + last_parts[lon_step]:
            copy.wait_send()
    for copy in row_copies + [own_pass, table_copy]:
        copy.wait_send()


def per_device(
    sizes,
    tokens,
    norm1_gain,
    qkv_weight,
    proj_weight,
    earth_bias,
    norm2_gain,
    fc1_weight,
    fc2_weight,
):
    assert tokens.shape[:3] == (WLV, WLA, WLO)
    assert sizes[0] == 2 and sizes[2] > 3 and earth_bias.shape[0] == 2
    features = tokens.shape[-1]
    assert LANES + LANES // 2 == features
    operands = (
        tokens.transpose(1, 2, 0, 3),
        norm1_gain.reshape(1, -1),
        earth_bias.transpose(1, 2, 0, 3),
        jnp.asarray(toeplitz_matrix(), jnp.bfloat16),
        qkv_weight,
        proj_weight,
        norm2_gain.reshape(1, -1),
        fc1_weight,
        fc2_weight.T,
    )
    assert len(operands) == OPERANDS
    blended = pl.pallas_call(
        functools.partial(kernel, sizes),
        out_shape=jax.ShapeDtypeStruct(operands[0].shape, jnp.bfloat16),
        in_specs=[pl.BlockSpec(memory_space=pltpu.HBM)] * OPERANDS,
        out_specs=pl.BlockSpec(memory_space=pltpu.VMEM),
        scratch_shapes=[
            *[pltpu.VMEM(operand.shape, operand.dtype) for operand in operands],
            pltpu.VMEM((2, 2, SIDE, features), jnp.float32),
            pltpu.VMEM((4, KINDS, 4, PITCH, LANES), jnp.bfloat16),
            pltpu.VMEM((WLV, ROWS, earth_bias.shape[-1]), jnp.float32),
            pltpu.VMEM((3 * ROWS, SECTION), jnp.bfloat16),
            pltpu.VMEM((3 * ROWS, SECTION), jnp.bfloat16),
            pltpu.VMEM((2, 2, 3, STACK, LANES), jnp.float32),
            pltpu.VMEM((2, 2, 2 * LANES, features), jnp.bfloat16),
            pltpu.VMEM((2, 4, STACK, features), jnp.bfloat16),
            pltpu.VMEM((4, 3 * LATS, features), jnp.bfloat16),
            pltpu.VMEM((4, 3 * LATS, features), jnp.bfloat16),
            pltpu.VMEM((2, 2, 2 * SIDE, LANES), jnp.float32),
            pltpu.SemaphoreType.DMA((2, message_count(sizes))),
            pltpu.SemaphoreType.DMA((OPERANDS - 1 + WLA // LOAD_ROWS,)),
            pltpu.SemaphoreType.REGULAR,
            pltpu.VMEM((features, 2 * LANES), jnp.bfloat16),
        ],
        compiler_params=pltpu.CompilerParams(
            collective_id=0, has_side_effects=True, vmem_limit_bytes=48 * 1024 * 1024
        ),
    )(*[pltpu.with_memory_space_constraint(x, pltpu.HBM) for x in operands])
    return blended.transpose(2, 0, 1, 3)


def solution(mesh):
    placed = (
        P("lev", "lat", "lon", None),
        P(),
        P(),
        P(),
        P(None, "lat", None, None),
        P(),
        P(),
        P(),
    )
    return jax.shard_map(
        functools.partial(per_device, tuple(mesh.shape[axis] for axis in AXES)),
        mesh=mesh,
        in_specs=placed,
        out_specs=P("lev", "lat", "lon", None),
        check_vma=False,
    )
```

```python
import functools

import jax
import jax.numpy as jnp
import numpy as np
from jax import lax
from jax.experimental import pallas as pl
from jax.experimental.pallas import tpu as pltpu
from jax.sharding import PartitionSpec as P

HEADS = 6
WLV = 2
WLA = 6
WLO = 12
HALF_LA = WLA // 2
HALF_LO = WLO // 2
OCT = HALF_LA * HALF_LO
PITCH = 24
SIDE = 2 * PITCH
LATS = 2 * SIDE
SPAN = 2 * WLO - 1
CHUNK = WLA * SPAN
ROWS = 8
LANES = 128
AXES = ("lev", "lat", "lon")
OPERANDS = 9
STACK = HEADS * PITCH
SECTION = HALF_LA * CHUNK
KINDS = 5
LOAD_ROWS = 2

norm_eps = 1e-05


def octant_row(lat, lon):
    return lat // HALF_LA * PITCH + lat % HALF_LA * HALF_LO + lon % HALF_LO


def toeplitz_matrix():
    pick = np.zeros((CHUNK, WLO * LANES), np.float32)
    for lon in range(WLO):
        for key_lat in range(WLA):
            for key_lon in range(WLO):
                column = lon * LANES + key_lon // HALF_LO * SIDE + octant_row(key_lat, key_lon)
                pick[key_lat * SPAN + lon - key_lon + WLO - 1, column] = 1
    return pick


def matmul(a, b):
    return jnp.dot(a, b, preferred_element_type=jnp.float32)


def lat_moves(size, at):
    stay = (0, 1, 1, 2)
    if size == 2:
        return (stay, (1, 2 - at, 3 * at, 1))
    return (stay, (1, 2, 0, 1), (-1, 1, 3, 1))


def lon_moves():
    return (
        (1, slice(2, 3), slice(0, 1)),
        (-1, slice(1, 2), slice(3, 4)),
        (0, slice(1, 3), slice(1, 3)),
    )


def message_count(sizes):
    lats = len(lat_moves(sizes[1], 0))
    return 4 * lats + (lats - 1) + 3 + 1 + lats


def kernel(sizes, *refs):
    operands, out_ref, held = refs[:OPERANDS], refs[OPERANDS], refs[OPERANDS + 1 : -15]
    (
        own,
        cells,
        tables,
        chunks_out,
        chunks_in,
        bias,
        weights,
        stacked,
        keys,
        values,
        rows_out,
        sems,
        load_sems,
        ready,
        means,
    ) = refs[-15:]
    token_loads = [
        pltpu.make_async_copy(
            operands[0].at[pl.ds(part * LOAD_ROWS, LOAD_ROWS)],
            held[0].at[pl.ds(part * LOAD_ROWS, LOAD_ROWS)],
            load_sems.at[OPERANDS - 1 + part if part else 0],
        )
        for part in range(WLA // LOAD_ROWS)
    ]
    loads = token_loads[:1] + [
        pltpu.make_async_copy(operands[i], held[i], load_sems.at[i]) for i in range(1, OPERANDS)
    ]
    for load in token_loads + loads[1:]:
        load.start()
    (
        tokens_ref,
        gain1_ref,
        table_ref,
        pick_ref,
        qkv_ref,
        proj_ref,
        gain2_ref,
        fc1_ref,
        fc2_ref,
    ) = held
    lev, lat, lon = where = [lax.axis_index(axis) for axis in AXES]
    features = own.shape[-1]
    slots = (lev, 1 - lev)

    def device(steps):
        return {
            axis: lax.rem(at + step + size, size)
            for axis, at, step, size in zip(AXES, where, steps, sizes)
        }

    moves = lat_moves(sizes[1], lat)
    per_side = 2 * len(moves)

    def remote(source, target, index, there):
        return pltpu.make_async_remote_copy(
            src_ref=source,
            dst_ref=target,
            send_sem=sems.at[0, index],
            recv_sem=sems.at[1, index],
            device_id=there,
            device_id_type=pl.DeviceIdType.MESH,
        )

    def part_of(columns, kinds, octants):
        return cells.at[columns, kinds, octants, 0:OCT, :]

    tail_kinds, plain_kind, passed_kinds = slice(1, 3), slice(0, 1), slice(3, 5)
    first_parts, last_parts, peers = {}, {}, {}
    for side, (lon_step, lon_from, lon_to) in enumerate(lon_moves()[:2]):
        first_parts[lon_step], last_parts[lon_step], peers[lon_step] = [], [], []
        for at, (lat_step, lat_from, lat_to, octants) in enumerate(moves):
            there = device((0, lat_step, lon_step))
            peers[lon_step].append(there)
            for part, kinds in enumerate((tail_kinds, plain_kind)):
                (first_parts, last_parts)[part][lon_step].append(
                    remote(
                        part_of(lon_from, kinds, pl.ds(lat_from, octants)),
                        part_of(lon_to, kinds, pl.ds(lat_to, octants)),
                        side * per_side + at * 2 + part,
                        there,
                    )
                )
    row_copies, row_peers = [], []
    for at, (lat_step, lat_from, lat_to, octants) in enumerate(moves[1:]):
        row_peers.append(device((0, lat_step, 0)))
        row_copies.append(
            remote(
                part_of(slice(1, 3), slice(0, 3), pl.ds(lat_from, octants)),
                part_of(slice(1, 3), slice(0, 3), pl.ds(lat_to, octants)),
                2 * per_side + at,
                row_peers[-1],
            )
        )
    partner = device((1, 0, 0))
    passed = 2 * per_side + len(row_copies)
    used = pl.ds(1 - lat, 3) if sizes[1] == 2 else slice(0, 4)

    def pass_on(columns, index):
        return remote(
            part_of(columns, tail_kinds, used),
            part_of(columns, passed_kinds, used),
            passed + index,
            partner,
        )

    own_pass = pass_on(slice(1, 3), 2)
    table_copy = remote(chunks_out, chunks_in, passed + 3, device((0, 1, 0)))
    crossings, cross_peers = {}, {}
    for lon_step, lon_from, lon_to in lon_moves()[:2]:
        crossings[lon_step], cross_peers[lon_step] = [], []
        for at, (lat_step, lat_from, lat_to, octants) in enumerate(moves):
            there = device((1, lat_step, lon_step))
            cross_peers[lon_step].append(there)
            crossings[lon_step].append(
                remote(
                    part_of(lon_from, tail_kinds, pl.ds(lat_from, octants)),
                    part_of(lon_to, passed_kinds, pl.ds(lat_to, octants)),
                    passed + 4 + at,
                    there,
                )
            )

    barrier = pltpu.get_barrier_semaphore()
    first_lon, last_lon = lon == 0, lon == sizes[2] - 1
    before_last = lon == sizes[2] - 2
    at_wrap = first_lon | last_lon

    def tell(semaphore, group):
        for there in group:
            pl.semaphore_signal(
                semaphore, inc=1, device_id=there, device_id_type=pl.DeviceIdType.MESH
            )

    def start(*groups):
        for group in groups:
            for copy in group:
                copy.start()

    wrapped = len(moves)
    greetings = len(row_peers) + 1 + 2 * wrapped
    tell(barrier, peers[-1])
    pl.when(first_lon)(lambda: tell(barrier, cross_peers[-1]))
    pl.when(last_lon)(lambda: tell(barrier, [device((1, 0, -1))]))
    pl.when(jnp.logical_not(last_lon))(lambda: tell(barrier, row_peers + [partner]))
    pl.when(jnp.logical_not(last_lon | before_last))(lambda: tell(barrier, peers[1]))

    cells[:, :, :, OCT:, :] = jnp.zeros((4, KINDS, 4, PITCH - OCT, LANES), jnp.bfloat16)
    for pad in (OCT, PITCH + OCT):
        own[:, :, pad : pad + PITCH - OCT, :] = jnp.zeros(
            (2, 2, PITCH - OCT, features), jnp.float32
        )
    if sizes[1] == 2:
        blank = jnp.zeros((4, KINDS, PITCH, LANES), jnp.bfloat16)

        def clear_low():
            cells[:, :, 0] = blank

        def clear_high():
            cells[:, :, 3] = blank

        pl.when(lat == 0)(clear_low)
        pl.when(lat == 1)(clear_high)

    @pl.when(last_lon)
    def _():
        pl.semaphore_wait(barrier, 2 * wrapped)
        tell(ready, peers[1] + cross_peers[1])

    for a in range(WLA):
        if a % LOAD_ROWS == 0:
            token_loads[a // LOAD_ROWS].wait()
        for o in range(WLO):
            cell = tokens_ref[a, o].astype(jnp.float32)
            row = octant_row(a, o)
            for side in range(WLV):
                own[o // HALF_LO, slots[side], row : row + 1, :] = cell[side : side + 1]
    loads[1].wait()
    raw = own[...].reshape(4 * SIDE, features)
    averages = jnp.mean(raw, axis=-1, keepdims=True)
    normed = raw - averages
    scales = lax.rsqrt(jnp.mean(normed * normed, axis=-1, keepdims=True) + norm_eps)
    normed = normed * scales * gain1_ref[...]
    lower = lax.broadcasted_iota(jnp.int32, (SIDE, LANES), 1) < features - LANES
    tail_gain = jnp.concatenate([gain1_ref[:, LANES:]] * 2, axis=1)
    for half in range(2):
        pair = [slice(at, at + SIDE) for at in (half * 2 * SIDE, (half * 2 + 1) * SIDE)]
        tails = jnp.concatenate([raw[rows, LANES:] for rows in pair], axis=1)
        average, by = (
            jnp.where(lower, found[pair[0]], found[pair[1]]) for found in (averages, scales)
        )
        tails = (tails - average) * by * tail_gain
        for kind, block in enumerate((normed[pair[0], :LANES], normed[pair[1], :LANES], tails)):
            cells[1 + half, kind, 1:3] = block.reshape(2, PITCH, LANES).astype(jnp.bfloat16)
    normed = normed.astype(jnp.bfloat16)

    def over_wrap(lon_step, at_lat, at_lev):
        own = [first_parts[lon_step], last_parts[lon_step]]
        for to_lat in range(2):
            index = at_lat ^ to_lat
            groups = [own, [crossings[lon_step]]]
            for group in groups[at_lev], groups[1 - at_lev]:
                for copies in group:
                    copies[index].start()

    def send_over_wrap(lon_step, order):
        if sizes[1] != 2:
            start(first_parts[lon_step], last_parts[lon_step], crossings[lon_step])
            return
        for at_lat in range(2):
            for at_lev in range(2):
                pl.when((lat == at_lat) & (lev == at_lev))(
                    functools.partial(over_wrap, lon_step, at_lat, at_lev ^ order)
                )

    pl.when(last_lon)(lambda: send_over_wrap(1, 0))

    @pl.when(jnp.logical_not(last_lon))
    def _():
        expected = jnp.where(first_lon, greetings - wrapped, greetings)
        pl.semaphore_wait(barrier, jnp.where(before_last, greetings + 1, expected))
        pl.when(before_last)(lambda: tell(ready, peers[1]))
        pl.when(jnp.logical_not(first_lon))(lambda: start(first_parts[-1], last_parts[-1]))
        start(row_copies, first_parts[1], last_parts[1])

    loads[2].wait()
    tables[...] = jnp.zeros_like(tables)
    for head in range(HEADS):
        pair = table_ref[0, head].astype(jnp.float32)
        for kind in range(WLV):
            tables[kind, head : head + 1, :] = pair[kind : kind + 1]

    def section(kind, query_lev, key_lev, side):
        at = (query_lev * WLV + key_lev) * WLA * CHUNK + side * SECTION
        return tables[kind, :, at : at + SECTION]

    def sections(side):
        found = [
            jnp.where(lev == 0, section(kind, *low, side), section(kind, *high, side))
            for kind, low, high in ((1, (1, 1), (0, 0)), (0, (0, 0), (1, 1)), (0, (0, 1), (1, 0)))
        ]
        return jnp.concatenate(found, axis=0)

    chunks_out[...] = sections(1).astype(jnp.bfloat16)
    pl.when(jnp.logical_not(last_lon))(table_copy.start)
    own_chunks = sections(0)

    lane = lax.broadcasted_iota(jnp.int32, (ROWS, LANES), 1)
    lat_side = lane % SIDE // PITCH
    real = (lane < LATS) & (lane % PITCH < OCT)
    partner_out = (lat == 0, lat == sizes[1] - 1)

    def fill_bias(half, found):
        chunk_rows = jnp.concatenate(
            [found[:, step * CHUNK : (step + 1) * CHUNK] for step in range(HALF_LA)], axis=0
        )
        spread = matmul(chunk_rows.astype(jnp.bfloat16), pick_ref[...])
        allowed = real & ((lat_side != half) | jnp.logical_not(partner_out[half]))
        for step in range(HALF_LA):
            for kind in range(3):
                at = (step * 3 + kind) * ROWS
                for o in range(WLO):
                    tile = spread[at : at + ROWS, o * LANES : (o + 1) * LANES]
                    tile = jnp.where(allowed, tile, -1e30)
                    bias[
                        1 - o // HALF_LO,
                        half,
                        kind,
                        pl.ds(step * HALF_LO + o % HALF_LO, HEADS, stride=PITCH),
                        :,
                    ] = tile[:HEADS]

    loads[3].wait()
    fill_bias(1, own_chunks)

    loads[4].wait()
    for part in range(2):
        weight = qkv_ref[:, (part + 1) * features : (part + 2) * features]
        blank_rows = jnp.zeros((features - LANES, features), jnp.bfloat16)
        for slot in range(2):
            weights[part, slot, :LANES] = weight[:LANES]
            pieces = (weight[LANES:], blank_rows)
            for place in range(2):
                at = LANES + place * (features - LANES)
                weights[part, slot, at : at + features - LANES] = pieces[place ^ slot]
    queries = matmul(normed, qkv_ref[:, :features])
    head_of = lax.broadcasted_iota(jnp.int32, (PITCH, features), 1) // (features // HEADS)
    for octant in range(8):
        rows = queries[octant * PITCH : (octant + 1) * PITCH]
        stacked[octant // 4, octant % 4] = jnp.concatenate(
            [jnp.where(head_of == head, rows, 0.0) for head in range(HEADS)], axis=0
        ).astype(jnp.bfloat16)

    def project(column):
        plain, paired, tails, passed_on, passed_tails = (
            cells[column, kind].reshape(LATS, LANES) for kind in range(KINDS)
        )
        plain = jnp.concatenate([plain, tails], axis=1)
        paired = jnp.concatenate(
            [
                jnp.concatenate([paired, tails], axis=1),
                jnp.concatenate([passed_on, passed_tails], axis=1),
            ],
            axis=0,
        )
        for part, kept in enumerate((keys, values)):
            kept[column, :LATS] = matmul(plain, weights[part, 0]).astype(jnp.bfloat16)
            kept[column, LATS:] = matmul(paired, weights[part, 1]).astype(jnp.bfloat16)

    def receive(phase, part):
        for at, (_, lat_from, lat_to, octants) in enumerate(moves):
            kinds = (tail_kinds, plain_kind)[part]
            remote(
                part_of(slice(1, 2), kinds, pl.ds(lat_from, octants)),
                part_of(pl.ds(3 * phase, 1), kinds, pl.ds(lat_to, octants)),
                phase * per_side + at * 2 + part,
                partner,
            ).wait_recv()

    def relay(phase):
        receive(phase, 0)
        pass_on(pl.ds(3 * phase, 1), phase).start()

    def relayed(phase):
        pass_on(pl.ds(3 * phase, 1), phase).wait_recv()

    near = jnp.where(last_lon, 0, 1)

    @pl.when(last_lon)
    def _():
        pl.semaphore_wait(ready, wrapped)
        start(row_copies, [table_copy], first_parts[-1], last_parts[-1])

    for copy in row_copies:
        copy.wait_recv()
    own_pass.start()
    relay(near)
    pl.when(jnp.logical_not(at_wrap))(lambda: relay(1 - near))
    @pl.when(first_lon)
    def _():
        pl.semaphore_wait(ready, 2 * wrapped)
        send_over_wrap(-1, 1)

    table_copy.wait_recv()
    fill_bias(0, chunks_in[...].astype(jnp.float32))
    own_pass.wait_recv()
    for column in (1, 2):
        project(column)
    for load in loads[5:]:
        load.wait()
    row_mean = jnp.mean(proj_ref[...].astype(jnp.float32), axis=-1, keepdims=True)
    high_part = row_mean.astype(jnp.bfloat16)
    low_part = (row_mean - high_part.astype(jnp.float32)).astype(jnp.bfloat16)
    for part, column in enumerate((high_part, low_part)):
        means[:, part * LANES : (part + 1) * LANES] = jnp.broadcast_to(column, (features, LANES))

    scale = (features // HEADS) ** (-0.5)
    rest = jnp.zeros((LANES - LATS, features), jnp.bfloat16)

    def window_rows(held_rows, phase, slot, half):
        at = slot * LATS + half * SIDE
        pieces = [held_rows[2 * phase + side, at : at + SIDE, :] for side in range(2)]
        return pieces + [rest]

    def attend(phases):
        octants = [(p, slot, half) for p in phases for slot in range(2) for half in range(2)]
        slot_keys = ((0,), (1, 2))

        def window(held_rows, phase, slot, half):
            return jnp.concatenate(
                [r for s in slot_keys[slot] for r in window_rows(held_rows, phase, s, half)], axis=0
            )

        scores = [
            lax.dot_general(
                stacked[phase, slot * 2 + half],
                window(keys, phase, slot, half),
                (((1,), (1,)), ((), ())),
                preferred_element_type=jnp.float32,
            )
            for phase, slot, half in octants
        ]
        shares, totals = [], []
        for (phase, slot, half), products in zip(octants, scores):
            added = jnp.concatenate([bias[phase, half, s] for s in slot_keys[slot]], axis=1)
            products = products * scale + added
            weight = jnp.exp(products - jnp.max(products, axis=-1, keepdims=True))
            shares.append(weight.astype(jnp.bfloat16))
            totals.append(jnp.sum(weight, axis=-1, keepdims=True))
        mixes = [
            matmul(weight, window(values, phase, slot, half))
            for (phase, slot, half), weight in zip(octants, shares)
        ]
        found = []
        for mixed, total in zip(mixes, totals):
            mixed = mixed * (1.0 / total)
            found.append(
                sum(
                    jnp.where(head_of == head, mixed[head * PITCH : (head + 1) * PITCH], 0.0)
                    for head in range(HEADS)
                )
            )
        context = jnp.concatenate(found, axis=0).astype(jnp.bfloat16)
        tokens = jnp.concatenate([own[p].reshape(4 * PITCH, features) for p in phases], axis=0)
        average = matmul(context, means[...])
        average = average[:, :LANES] + average[:, LANES:]
        average = average + jnp.mean(tokens, axis=-1, keepdims=True)
        first = tokens + matmul(context, proj_ref[...])
        centered = first - jnp.concatenate([average, average[:, : features - LANES]], axis=1)
        variance = jnp.mean(centered * centered, axis=-1, keepdims=True)
        normed_two = centered * lax.rsqrt(variance + norm_eps) * gain2_ref[...]
        normed_two = normed_two.astype(jnp.bfloat16)
        hidden = matmul(normed_two, fc1_ref[...])
        hidden = hidden * (1.0 + lax.erf(hidden * np.float32(0.5**0.5)))
        blended = first + 0.5 * lax.dot_general(
            hidden.astype(jnp.bfloat16),
            fc2_ref[...],
            (((1,), (1,)), ((), ())),
            preferred_element_type=jnp.float32,
        )
        for place, phase in enumerate(phases):
            at = place * 2 * SIDE
            for slot in range(2):
                rows = blended[at + slot * SIDE : at + (slot + 1) * SIDE]
                target = pl.ds(slots[slot], SIDE, stride=2)
                rows_out[place, 0, target, :] = rows[:, :LANES]
                rows_out[place, 1, target, : features - LANES] = rows[:, LANES:]
            for a in range(WLA):
                for o in range(HALF_LO):
                    row = 2 * octant_row(a, o)
                    pieces = rows_out[place, :, row : row + 2, :].astype(jnp.bfloat16)
                    out_ref[a, phase * HALF_LO + o, :, :LANES] = pieces[0]
                    out_ref[a, phase * HALF_LO + o, :, LANES:] = pieces[1, :, : features - LANES]

    def run_phase(step, _):
        phase = jnp.where(step == 0, near, 1 - near)
        pl.when(step == 0)(lambda: relayed(phase))

        @pl.when(step == 1)
        def _():
            receive(phase, 0)
            for copy in crossings[1]:
                copy.wait_recv()

        receive(phase, 1)
        project(3 * phase)
        attend((phase,))
        return 0

    @pl.when(at_wrap)
    def _():
        lax.fori_loop(0, 2, run_phase, 0)
        pass_on(pl.ds(3 * near, 1), near).wait_send()
        for copy in crossings[1]:
            copy.wait_send()

    @pl.when(jnp.logical_not(at_wrap))
    def _():
        for phase in (1, 0):
            receive(phase, 1)
            relayed(phase)
            project(3 * phase)
        attend((0, 1))
        for phase in range(2):
            pass_on(slice(3 * phase, 3 * phase + 1), phase).wait_send()

    for lon_step in (1, -1):
        for copy in first_parts[lon_step] + last_parts[lon_step]:
            copy.wait_send()
    for copy in row_copies + [own_pass, table_copy]:
        copy.wait_send()


def per_device(
    sizes,
    tokens,
    norm1_gain,
    qkv_weight,
    proj_weight,
    earth_bias,
    norm2_gain,
    fc1_weight,
    fc2_weight,
):
    assert tokens.shape[:3] == (WLV, WLA, WLO)
    assert sizes[0] == 2 and sizes[2] > 3 and earth_bias.shape[0] == 2
    features = tokens.shape[-1]
    assert LANES + LANES // 2 == features
    operands = (
        tokens.transpose(1, 2, 0, 3),
        norm1_gain.reshape(1, -1),
        earth_bias.transpose(1, 2, 0, 3),
        jnp.asarray(toeplitz_matrix(), jnp.bfloat16),
        qkv_weight,
        proj_weight,
        norm2_gain.reshape(1, -1),
        fc1_weight,
        fc2_weight.T,
    )
    assert len(operands) == OPERANDS
    blended = pl.pallas_call(
        functools.partial(kernel, sizes),
        out_shape=jax.ShapeDtypeStruct(operands[0].shape, jnp.bfloat16),
        in_specs=[pl.BlockSpec(memory_space=pltpu.HBM)] * OPERANDS,
        out_specs=pl.BlockSpec(memory_space=pltpu.VMEM),
        scratch_shapes=[
            *[pltpu.VMEM(operand.shape, operand.dtype) for operand in operands],
            pltpu.VMEM((2, 2, SIDE, features), jnp.float32),
            pltpu.VMEM((4, KINDS, 4, PITCH, LANES), jnp.bfloat16),
            pltpu.VMEM((WLV, ROWS, earth_bias.shape[-1]), jnp.float32),
            pltpu.VMEM((3 * ROWS, SECTION), jnp.bfloat16),
            pltpu.VMEM((3 * ROWS, SECTION), jnp.bfloat16),
            pltpu.VMEM((2, 2, 3, STACK, LANES), jnp.float32),
            pltpu.VMEM((2, 2, 2 * LANES, features), jnp.bfloat16),
            pltpu.VMEM((2, 4, STACK, features), jnp.bfloat16),
            pltpu.VMEM((4, 3 * LATS, features), jnp.bfloat16),
            pltpu.VMEM((4, 3 * LATS, features), jnp.bfloat16),
            pltpu.VMEM((2, 2, 2 * SIDE, LANES), jnp.float32),
            pltpu.SemaphoreType.DMA((2, message_count(sizes))),
            pltpu.SemaphoreType.DMA((OPERANDS - 1 + WLA // LOAD_ROWS,)),
            pltpu.SemaphoreType.REGULAR,
            pltpu.VMEM((features, 2 * LANES), jnp.bfloat16),
        ],
        compiler_params=pltpu.CompilerParams(
            collective_id=0, has_side_effects=True, vmem_limit_bytes=48 * 1024 * 1024
        ),
    )(*[pltpu.with_memory_space_constraint(x, pltpu.HBM) for x in operands])
    return blended.transpose(2, 0, 1, 3)


def solution(mesh):
    placed = (
        P("lev", "lat", "lon", None),
        P(),
        P(),
        P(),
        P(None, "lat", None, None),
        P(),
        P(),
        P(),
    )
    return jax.shard_map(
        functools.partial(per_device, tuple(mesh.shape[axis] for axis in AXES)),
        mesh=mesh,
        in_specs=placed,
        out_specs=P("lev", "lat", "lon", None),
        check_vma=False,
    )
```

```python
import functools

import jax
import jax.numpy as jnp
import numpy as np
from jax import lax
from jax.experimental import pallas as pl
from jax.experimental.pallas import tpu as pltpu
from jax.sharding import PartitionSpec as P

HEADS = 6
WLV = 2
WLA = 6
WLO = 12
HALF_LA = WLA // 2
HALF_LO = WLO // 2
OCT = HALF_LA * HALF_LO
PITCH = 24
SIDE = 2 * PITCH
LATS = 2 * SIDE
SPAN = 2 * WLO - 1
CHUNK = WLA * SPAN
ROWS = 8
LANES = 128
AXES = ("lev", "lat", "lon")
OPERANDS = 9
STACK = HEADS * PITCH
SECTION = HALF_LA * CHUNK
KINDS = 5
LOAD_ROWS = 2

norm_eps = 1e-05


def octant_row(lat, lon):
    return lat // HALF_LA * PITCH + lat % HALF_LA * HALF_LO + lon % HALF_LO


def toeplitz_matrix():
    pick = np.zeros((CHUNK, WLO * LANES), np.float32)
    for lon in range(WLO):
        for key_lat in range(WLA):
            for key_lon in range(WLO):
                column = lon * LANES + key_lon // HALF_LO * SIDE + octant_row(key_lat, key_lon)
                pick[key_lat * SPAN + lon - key_lon + WLO - 1, column] = 1
    return pick


def matmul(a, b):
    return jnp.dot(a, b, preferred_element_type=jnp.float32)


def lat_moves(size, at):
    stay = (0, 1, 1, 2)
    if size == 2:
        return (stay, (1, 2 - at, 3 * at, 1))
    return (stay, (1, 2, 0, 1), (-1, 1, 3, 1))


def lon_moves():
    return (
        (1, slice(2, 3), slice(0, 1)),
        (-1, slice(1, 2), slice(3, 4)),
        (0, slice(1, 3), slice(1, 3)),
    )


def message_count(sizes):
    lats = len(lat_moves(sizes[1], 0))
    return 4 * lats + (lats - 1) + 3 + 1 + lats


def kernel(sizes, *refs):
    operands, out_ref, held = refs[:OPERANDS], refs[OPERANDS], refs[OPERANDS + 1 : -15]
    (
        own,
        cells,
        tables,
        chunks_out,
        chunks_in,
        bias,
        weights,
        stacked,
        keys,
        values,
        rows_out,
        sems,
        load_sems,
        ready,
        means,
    ) = refs[-15:]
    token_loads = [
        pltpu.make_async_copy(
            operands[0].at[pl.ds(part * LOAD_ROWS, LOAD_ROWS)],
            held[0].at[pl.ds(part * LOAD_ROWS, LOAD_ROWS)],
            load_sems.at[OPERANDS - 1 + part if part else 0],
        )
        for part in range(WLA // LOAD_ROWS)
    ]
    loads = token_loads[:1] + [
        pltpu.make_async_copy(operands[i], held[i], load_sems.at[i]) for i in range(1, OPERANDS)
    ]
    for load in token_loads + loads[1:]:
        load.start()
    (
        tokens_ref,
        gain1_ref,
        table_ref,
        pick_ref,
        qkv_ref,
        proj_ref,
        gain2_ref,
        fc1_ref,
        fc2_ref,
    ) = held
    lev, lat, lon = where = [lax.axis_index(axis) for axis in AXES]
    features = own.shape[-1]
    slots = (lev, 1 - lev)

    def device(steps):
        return {
            axis: lax.rem(at + step + size, size)
            for axis, at, step, size in zip(AXES, where, steps, sizes)
        }

    moves = lat_moves(sizes[1], lat)
    per_side = 2 * len(moves)

    def remote(source, target, index, there):
        return pltpu.make_async_remote_copy(
            src_ref=source,
            dst_ref=target,
            send_sem=sems.at[0, index],
            recv_sem=sems.at[1, index],
            device_id=there,
            device_id_type=pl.DeviceIdType.MESH,
        )

    def part_of(columns, kinds, octants):
        return cells.at[columns, kinds, octants, 0:OCT, :]

    tail_kinds, plain_kind, passed_kinds = slice(1, 3), slice(0, 1), slice(3, 5)
    first_parts, last_parts, peers = {}, {}, {}
    for side, (lon_step, lon_from, lon_to) in enumerate(lon_moves()[:2]):
        first_parts[lon_step], last_parts[lon_step], peers[lon_step] = [], [], []
        for at, (lat_step, lat_from, lat_to, octants) in enumerate(moves):
            there = device((0, lat_step, lon_step))
            peers[lon_step].append(there)
            for part, kinds in enumerate((tail_kinds, plain_kind)):
                (first_parts, last_parts)[part][lon_step].append(
                    remote(
                        part_of(lon_from, kinds, pl.ds(lat_from, octants)),
                        part_of(lon_to, kinds, pl.ds(lat_to, octants)),
                        side * per_side + at * 2 + part,
                        there,
                    )
                )
    row_copies, row_peers = [], []
    for at, (lat_step, lat_from, lat_to, octants) in enumerate(moves[1:]):
        row_peers.append(device((0, lat_step, 0)))
        row_copies.append(
            remote(
                part_of(slice(1, 3), slice(0, 3), pl.ds(lat_from, octants)),
                part_of(slice(1, 3), slice(0, 3), pl.ds(lat_to, octants)),
                2 * per_side + at,
                row_peers[-1],
            )
        )
    partner = device((1, 0, 0))
    passed = 2 * per_side + len(row_copies)
    used = pl.ds(1 - lat, 3) if sizes[1] == 2 else slice(0, 4)

    def pass_on(columns, index):
        return remote(
            part_of(columns, tail_kinds, used),
            part_of(columns, passed_kinds, used),
            passed + index,
            partner,
        )

    own_pass = pass_on(slice(1, 3), 2)
    table_copy = remote(chunks_out, chunks_in, passed + 3, device((0, 1, 0)))
    crossings, cross_peers = {}, {}
    for lon_step, lon_from, lon_to in lon_moves()[:2]:
        crossings[lon_step], cross_peers[lon_step] = [], []
        for at, (lat_step, lat_from, lat_to, octants) in enumerate(moves):
            there = device((1, lat_step, lon_step))
            cross_peers[lon_step].append(there)
            crossings[lon_step].append(
                remote(
                    part_of(lon_from, tail_kinds, pl.ds(lat_from, octants)),
                    part_of(lon_to, passed_kinds, pl.ds(lat_to, octants)),
                    passed + 4 + at,
                    there,
                )
            )

    barrier = pltpu.get_barrier_semaphore()
    first_lon, last_lon = lon == 0, lon == sizes[2] - 1
    before_last = lon == sizes[2] - 2
    at_wrap = first_lon | last_lon

    def tell(semaphore, group):
        for there in group:
            pl.semaphore_signal(
                semaphore, inc=1, device_id=there, device_id_type=pl.DeviceIdType.MESH
            )

    def start(*groups):
        for group in groups:
            for copy in group:
                copy.start()

    wrapped = len(moves)
    greetings = len(row_peers) + 1 + 2 * wrapped
    tell(barrier, peers[-1])
    pl.when(first_lon)(lambda: tell(barrier, cross_peers[-1]))
    pl.when(last_lon)(lambda: tell(barrier, [device((1, 0, -1))]))
    pl.when(jnp.logical_not(last_lon))(lambda: tell(barrier, row_peers + [partner]))
    pl.when(jnp.logical_not(last_lon | before_last))(lambda: tell(barrier, peers[1]))

    cells[:, :, :, OCT:, :] = jnp.zeros((4, KINDS, 4, PITCH - OCT, LANES), jnp.bfloat16)
    for pad in (OCT, PITCH + OCT):
        own[:, :, pad : pad + PITCH - OCT, :] = jnp.zeros(
            (2, 2, PITCH - OCT, features), jnp.float32
        )
    if sizes[1] == 2:
        blank = jnp.zeros((4, KINDS, PITCH, LANES), jnp.bfloat16)

        def clear_low():
            cells[:, :, 0] = blank

        def clear_high():
            cells[:, :, 3] = blank

        pl.when(lat == 0)(clear_low)
        pl.when(lat == 1)(clear_high)

    @pl.when(last_lon)
    def _():
        pl.semaphore_wait(barrier, 2 * wrapped)
        tell(ready, peers[1] + cross_peers[1])

    for a in range(WLA):
        if a % LOAD_ROWS == 0:
            token_loads[a // LOAD_ROWS].wait()
        for o in range(WLO):
            cell = tokens_ref[a, o].astype(jnp.float32)
            row = octant_row(a, o)
            for side in range(WLV):
                own[o // HALF_LO, slots[side], row : row + 1, :] = cell[side : side + 1]
    loads[1].wait()
    raw = own[...].reshape(4 * SIDE, features)
    averages = jnp.mean(raw, axis=-1, keepdims=True)
    normed = raw - averages
    scales = lax.rsqrt(jnp.mean(normed * normed, axis=-1, keepdims=True) + norm_eps)
    normed = normed * scales * gain1_ref[...]
    lower = lax.broadcasted_iota(jnp.int32, (SIDE, LANES), 1) < features - LANES
    tail_gain = jnp.concatenate([gain1_ref[:, LANES:]] * 2, axis=1)
    for half in range(2):
        pair = [slice(at, at + SIDE) for at in (half * 2 * SIDE, (half * 2 + 1) * SIDE)]
        tails = jnp.concatenate([raw[rows, LANES:] for rows in pair], axis=1)
        average, by = (
            jnp.where(lower, found[pair[0]], found[pair[1]]) for found in (averages, scales)
        )
        tails = (tails - average) * by * tail_gain
        for kind, block in enumerate((normed[pair[0], :LANES], normed[pair[1], :LANES], tails)):
            cells[1 + half, kind, 1:3] = block.reshape(2, PITCH, LANES).astype(jnp.bfloat16)
    normed = normed.astype(jnp.bfloat16)

    def over_wrap(lon_step, at_lat, at_lev):
        own = [first_parts[lon_step], last_parts[lon_step]]
        for to_lat in range(2):
            index = at_lat ^ to_lat
            groups = [own, [crossings[lon_step]]]
            for group in groups[at_lev], groups[1 - at_lev]:
                for copies in group:
                    copies[index].start()

    def send_over_wrap(lon_step, order):
        if sizes[1] != 2:
            start(first_parts[lon_step], last_parts[lon_step], crossings[lon_step])
            return
        for at_lat in range(2):
            for at_lev in range(2):
                pl.when((lat == at_lat) & (lev == at_lev))(
                    functools.partial(over_wrap, lon_step, at_lat, at_lev ^ order)
                )

    pl.when(last_lon)(lambda: send_over_wrap(1, 0))

    @pl.when(jnp.logical_not(last_lon))
    def _():
        expected = jnp.where(first_lon, greetings - wrapped, greetings)
        pl.semaphore_wait(barrier, jnp.where(before_last, greetings + 1, expected))
        pl.when(before_last)(lambda: tell(ready, peers[1]))
        pl.when(jnp.logical_not(first_lon))(lambda: start(first_parts[-1], last_parts[-1]))
        start(row_copies, first_parts[1], last_parts[1])

    loads[2].wait()
    tables[...] = jnp.zeros_like(tables)
    for head in range(HEADS):
        pair = table_ref[0, head].astype(jnp.float32)
        for kind in range(WLV):
            tables[kind, head : head + 1, :] = pair[kind : kind + 1]

    def section(kind, query_lev, key_lev, side):
        at = (query_lev * WLV + key_lev) * WLA * CHUNK + side * SECTION
        return tables[kind, :, at : at + SECTION]

    def sections(side):
        found = [
            jnp.where(lev == 0, section(kind, *low, side), section(kind, *high, side))
            for kind, low, high in ((1, (1, 1), (0, 0)), (0, (0, 0), (1, 1)), (0, (0, 1), (1, 0)))
        ]
        return jnp.concatenate(found, axis=0)

    chunks_out[...] = sections(1).astype(jnp.bfloat16)
    pl.when(jnp.logical_not(last_lon))(table_copy.start)
    own_chunks = sections(0)

    lane = lax.broadcasted_iota(jnp.int32, (ROWS, LANES), 1)
    lat_side = lane % SIDE // PITCH
    real = (lane < LATS) & (lane % PITCH < OCT)
    partner_out = (lat == 0, lat == sizes[1] - 1)

    def fill_bias(half, found):
        chunk_rows = jnp.concatenate(
            [found[:, step * CHUNK : (step + 1) * CHUNK] for step in range(HALF_LA)], axis=0
        )
        spread = matmul(chunk_rows.astype(jnp.bfloat16), pick_ref[...])
        allowed = real & ((lat_side != half) | jnp.logical_not(partner_out[half]))
        for step in range(HALF_LA):
            for kind in range(3):
                at = (step * 3 + kind) * ROWS
                for o in range(WLO):
                    tile = spread[at : at + ROWS, o * LANES : (o + 1) * LANES]
                    tile = jnp.where(allowed, tile, -1e30)
                    bias[
                        1 - o // HALF_LO,
                        half,
                        kind,
                        pl.ds(step * HALF_LO + o % HALF_LO, HEADS, stride=PITCH),
                        :,
                    ] = tile[:HEADS]

    loads[3].wait()
    fill_bias(1, own_chunks)

    loads[4].wait()
    for part in range(2):
        weight = qkv_ref[:, (part + 1) * features : (part + 2) * features]
        blank_rows = jnp.zeros((features - LANES, features), jnp.bfloat16)
        for slot in range(2):
            weights[part, slot, :LANES] = weight[:LANES]
            pieces = (weight[LANES:], blank_rows)
            for place in range(2):
                at = LANES + place * (features - LANES)
                weights[part, slot, at : at + features - LANES] = pieces[place ^ slot]
    queries = matmul(normed, qkv_ref[:, :features])
    head_of = lax.broadcasted_iota(jnp.int32, (PITCH, features), 1) // (features // HEADS)
    for octant in range(8):
        rows = queries[octant * PITCH : (octant + 1) * PITCH]
        stacked[octant // 4, octant % 4] = jnp.concatenate(
            [jnp.where(head_of == head, rows, 0.0) for head in range(HEADS)], axis=0
        ).astype(jnp.bfloat16)

    def project(column):
        plain, paired, tails, passed_on, passed_tails = (
            cells[column, kind].reshape(LATS, LANES) for kind in range(KINDS)
        )
        plain = jnp.concatenate([plain, tails], axis=1)
        paired = jnp.concatenate(
            [
                jnp.concatenate([paired, tails], axis=1),
                jnp.concatenate([passed_on, passed_tails], axis=1),
            ],
            axis=0,
        )
        for part, kept in enumerate((keys, values)):
            kept[column, :LATS] = matmul(plain, weights[part, 0]).astype(jnp.bfloat16)
            kept[column, LATS:] = matmul(paired, weights[part, 1]).astype(jnp.bfloat16)

    def receive(phase, part):
        for at, (_, lat_from, lat_to, octants) in enumerate(moves):
            kinds = (tail_kinds, plain_kind)[part]
            remote(
                part_of(slice(1, 2), kinds, pl.ds(lat_from, octants)),
                part_of(pl.ds(3 * phase, 1), kinds, pl.ds(lat_to, octants)),
                phase * per_side + at * 2 + part,
                partner,
            ).wait_recv()

    def relay(phase):
        receive(phase, 0)
        pass_on(pl.ds(3 * phase, 1), phase).start()

    def relayed(phase):
        pass_on(pl.ds(3 * phase, 1), phase).wait_recv()

    near = jnp.where(last_lon, 0, 1)

    @pl.when(last_lon)
    def _():
        pl.semaphore_wait(ready, wrapped)
        start(row_copies, [table_copy], first_parts[-1], last_parts[-1])

    for copy in row_copies:
        copy.wait_recv()
    own_pass.start()
    relay(near)
    pl.when(jnp.logical_not(at_wrap))(lambda: relay(1 - near))
    table_copy.wait_recv()
    fill_bias(0, chunks_in[...].astype(jnp.float32))
    own_pass.wait_recv()
    @pl.when(first_lon)
    def _():
        pl.semaphore_wait(ready, 2 * wrapped)
        send_over_wrap(-1, 1)

    for column in (1, 2):
        project(column)
    for load in loads[5:]:
        load.wait()
    row_mean = jnp.mean(proj_ref[...].astype(jnp.float32), axis=-1, keepdims=True)
    high_part = row_mean.astype(jnp.bfloat16)
    low_part = (row_mean - high_part.astype(jnp.float32)).astype(jnp.bfloat16)
    for part, column in enumerate((high_part, low_part)):
        means[:, part * LANES : (part + 1) * LANES] = jnp.broadcast_to(column, (features, LANES))

    scale = (features // HEADS) ** (-0.5)
    rest = jnp.zeros((LANES - LATS, features), jnp.bfloat16)

    def window_rows(held_rows, phase, slot, half):
        at = slot * LATS + half * SIDE
        pieces = [held_rows[2 * phase + side, at : at + SIDE, :] for side in range(2)]
        return pieces + [rest]

    def attend(phases):
        octants = [(p, slot, half) for p in phases for slot in range(2) for half in range(2)]
        slot_keys = ((0,), (1, 2))

        def window(held_rows, phase, slot, half):
            return jnp.concatenate(
                [r for s in slot_keys[slot] for r in window_rows(held_rows, phase, s, half)], axis=0
            )

        scores = [
            lax.dot_general(
                stacked[phase, slot * 2 + half],
                window(keys, phase, slot, half),
                (((1,), (1,)), ((), ())),
                preferred_element_type=jnp.float32,
            )
            for phase, slot, half in octants
        ]
        shares, totals = [], []
        for (phase, slot, half), products in zip(octants, scores):
            added = jnp.concatenate([bias[phase, half, s] for s in slot_keys[slot]], axis=1)
            products = products * scale + added
            weight = jnp.exp(products - jnp.max(products, axis=-1, keepdims=True))
            shares.append(weight.astype(jnp.bfloat16))
            totals.append(jnp.sum(weight, axis=-1, keepdims=True))
        mixes = [
            matmul(weight, window(values, phase, slot, half))
            for (phase, slot, half), weight in zip(octants, shares)
        ]
        found = []
        for mixed, total in zip(mixes, totals):
            mixed = mixed * (1.0 / total)
            found.append(
                sum(
                    jnp.where(head_of == head, mixed[head * PITCH : (head + 1) * PITCH], 0.0)
                    for head in range(HEADS)
                )
            )
        context = jnp.concatenate(found, axis=0).astype(jnp.bfloat16)
        tokens = jnp.concatenate([own[p].reshape(4 * PITCH, features) for p in phases], axis=0)
        average = matmul(context, means[...])
        average = average[:, :LANES] + average[:, LANES:]
        average = average + jnp.mean(tokens, axis=-1, keepdims=True)
        first = tokens + matmul(context, proj_ref[...])
        centered = first - jnp.concatenate([average, average[:, : features - LANES]], axis=1)
        variance = jnp.mean(centered * centered, axis=-1, keepdims=True)
        normed_two = centered * lax.rsqrt(variance + norm_eps) * gain2_ref[...]
        normed_two = normed_two.astype(jnp.bfloat16)
        hidden = matmul(normed_two, fc1_ref[...])
        hidden = hidden * (1.0 + lax.erf(hidden * np.float32(0.5**0.5)))
        blended = first + 0.5 * lax.dot_general(
            hidden.astype(jnp.bfloat16),
            fc2_ref[...],
            (((1,), (1,)), ((), ())),
            preferred_element_type=jnp.float32,
        )
        for place, phase in enumerate(phases):
            at = place * 2 * SIDE
            for slot in range(2):
                rows = blended[at + slot * SIDE : at + (slot + 1) * SIDE]
                target = pl.ds(slots[slot], SIDE, stride=2)
                rows_out[place, 0, target, :] = rows[:, :LANES]
                rows_out[place, 1, target, : features - LANES] = rows[:, LANES:]
            for a in range(WLA):
                for o in range(HALF_LO):
                    row = 2 * octant_row(a, o)
                    pieces = rows_out[place, :, row : row + 2, :].astype(jnp.bfloat16)
                    out_ref[a, phase * HALF_LO + o, :, :LANES] = pieces[0]
                    out_ref[a, phase * HALF_LO + o, :, LANES:] = pieces[1, :, : features - LANES]

    def run_phase(step, _):
        phase = jnp.where(step == 0, near, 1 - near)
        pl.when(step == 0)(lambda: relayed(phase))

        @pl.when(step == 1)
        def _():
            receive(phase, 0)
            for copy in crossings[1]:
                copy.wait_recv()

        receive(phase, 1)
        project(3 * phase)
        attend((phase,))
        return 0

    @pl.when(at_wrap)
    def _():
        lax.fori_loop(0, 2, run_phase, 0)
        pass_on(pl.ds(3 * near, 1), near).wait_send()
        for copy in crossings[1]:
            copy.wait_send()

    @pl.when(jnp.logical_not(at_wrap))
    def _():
        for phase in (1, 0):
            receive(phase, 1)
            relayed(phase)
            project(3 * phase)
        attend((0, 1))
        for phase in range(2):
            pass_on(slice(3 * phase, 3 * phase + 1), phase).wait_send()

    for lon_step in (1, -1):
        for copy in first_parts[lon_step] + last_parts[lon_step]:
            copy.wait_send()
    for copy in row_copies + [own_pass, table_copy]:
        copy.wait_send()


def per_device(
    sizes,
    tokens,
    norm1_gain,
    qkv_weight,
    proj_weight,
    earth_bias,
    norm2_gain,
    fc1_weight,
    fc2_weight,
):
    assert tokens.shape[:3] == (WLV, WLA, WLO)
    assert sizes[0] == 2 and sizes[2] > 3 and earth_bias.shape[0] == 2
    features = tokens.shape[-1]
    assert LANES + LANES // 2 == features
    operands = (
        tokens.transpose(1, 2, 0, 3),
        norm1_gain.reshape(1, -1),
        earth_bias.transpose(1, 2, 0, 3),
        jnp.asarray(toeplitz_matrix(), jnp.bfloat16),
        qkv_weight,
        proj_weight,
        norm2_gain.reshape(1, -1),
        fc1_weight,
        fc2_weight.T,
    )
    assert len(operands) == OPERANDS
    blended = pl.pallas_call(
        functools.partial(kernel, sizes),
        out_shape=jax.ShapeDtypeStruct(operands[0].shape, jnp.bfloat16),
        in_specs=[pl.BlockSpec(memory_space=pltpu.HBM)] * OPERANDS,
        out_specs=pl.BlockSpec(memory_space=pltpu.VMEM),
        scratch_shapes=[
            *[pltpu.VMEM(operand.shape, operand.dtype) for operand in operands],
            pltpu.VMEM((2, 2, SIDE, features), jnp.float32),
            pltpu.VMEM((4, KINDS, 4, PITCH, LANES), jnp.bfloat16),
            pltpu.VMEM((WLV, ROWS, earth_bias.shape[-1]), jnp.float32),
            pltpu.VMEM((3 * ROWS, SECTION), jnp.bfloat16),
            pltpu.VMEM((3 * ROWS, SECTION), jnp.bfloat16),
            pltpu.VMEM((2, 2, 3, STACK, LANES), jnp.float32),
            pltpu.VMEM((2, 2, 2 * LANES, features), jnp.bfloat16),
            pltpu.VMEM((2, 4, STACK, features), jnp.bfloat16),
            pltpu.VMEM((4, 3 * LATS, features), jnp.bfloat16),
            pltpu.VMEM((4, 3 * LATS, features), jnp.bfloat16),
            pltpu.VMEM((2, 2, 2 * SIDE, LANES), jnp.float32),
            pltpu.SemaphoreType.DMA((2, message_count(sizes))),
            pltpu.SemaphoreType.DMA((OPERANDS - 1 + WLA // LOAD_ROWS,)),
            pltpu.SemaphoreType.REGULAR,
            pltpu.VMEM((features, 2 * LANES), jnp.bfloat16),
        ],
        compiler_params=pltpu.CompilerParams(
            collective_id=0, has_side_effects=True, vmem_limit_bytes=48 * 1024 * 1024
        ),
    )(*[pltpu.with_memory_space_constraint(x, pltpu.HBM) for x in operands])
    return blended.transpose(2, 0, 1, 3)


def solution(mesh):
    placed = (
        P("lev", "lat", "lon", None),
        P(),
        P(),
        P(),
        P(None, "lat", None, None),
        P(),
        P(),
        P(),
    )
    return jax.shard_map(
        functools.partial(per_device, tuple(mesh.shape[axis] for axis in AXES)),
        mesh=mesh,
        in_specs=placed,
        out_specs=P("lev", "lat", "lon", None),
        check_vma=False,
    )
```
